128 devices in a mesh: blk: 8 (over x, z_hi), grp: 16 (over z_lo, y, core).
Axes of the slice: x: 4, y: 4, z: 4 (z_hi: 2, z_lo: 2; z = z_hi * 2 + z_lo), core: 2. Of those that a mesh axis runs over, the one named last changes fastest.
Arguments:
- frames: bfloat16 [16384, 8, 2048], P(('blk', 'grp')), may hold values from -6 to 6
- counts: int32 [16384], P(('blk', 'grp')), may hold values from 1 to 8
- positives: int32 [16384], P(('blk', 'grp')), may hold values from 0 to 16383, as said below
- w_first: bfloat16 [2048, 4096], P(None, 'grp'), may hold values from -0.125 to 0.125
- w_second: bfloat16 [4096, 256], P('grp'), may hold values from -0.09375 to 0.09375
Outputs:
- batch_loss: float32 [], replicated
- grad_first: float32 [2048, 4096], P(None, 'grp')
- grad_second: float32 [4096, 256], P('grp')
The draws below stay inside these ranges and needn't reach their ends.
Inputs may be any that keep to these rules, and one draw needn't show every extreme that they name: positives[positives[i]] = i and positives[i] != i for every clip i.
All inputs are finite; a program needn't handle non-finite values.
Results may differ from the reference program's by a relative error of at most 0.005.
The reference program's roundings to bfloat16 on the way count: a program that leaves them out, or rounds other values in their place, can miss the bound.
Values may be sent and summed in bfloat16 or wider, within the bound.
No kernel may reach another device: no remote copies, remote signals or barrier semaphores. Data moves between devices by JAX's collectives and lax.ppermute only.
A program may use at most 128 MiB of HBM per device.

```python
import jax
import jax.numpy as jnp
from jax import lax

C = 2048
H = 4096
E = 256
FRAMES = 8
GROUP_CLIPS = 2048
SEGMENT_COUNT = 16384


def draw_positives(key, part):
    order = jax.random.permutation(jax.random.fold_in(key, 17), SEGMENT_COUNT).astype(jnp.int32)
    first_half = order[0::2]
    second_half = order[1::2]
    paired = jnp.zeros((SEGMENT_COUNT,), jnp.int32).at[first_half].set(second_half).at[second_half].set(first_half)
    return paired.astype(jnp.int32)


def plant(drawn, key, low, high):
    place = [jax.random.randint(jax.random.fold_in(key, axis), (), 0, length) for axis, length in enumerate(drawn.shape)]
    main_axis = drawn.shape.index(max(drawn.shape))
    next_to = place[:main_axis] + [(place[main_axis] + 1) % drawn.shape[main_axis]] + place[main_axis + 1:]
    return drawn.at[tuple(place)].set(low).at[tuple(next_to)].set(high)


def levels(key, dims, shards, smallest, top_value):
    def one(position, parts):
        draws = jax.random.uniform(jax.random.fold_in(jax.random.fold_in(key, 6), position), (parts,), jnp.float32, smallest / len(shards), top_value / len(shards))
        return jnp.repeat(jnp.exp(draws), dims[position] // parts).reshape((-1,) + (1,) * (len(dims) - position - 1))

    level = one(*shards[0])
    for cut in shards[1:]:
        level = level * one(*cut)
    return level


def centred(key, dims, scale, reach, shards=(), kind=jnp.bfloat16):
    level = levels(key, dims, shards, -0.22, 0.18) if shards else 1.0
    values = jax.random.normal(key, dims, jnp.float32) * scale * level
    return jnp.minimum(jnp.maximum(values, -reach), reach).astype(kind)


def setup_inputs(seed: int = 0) -> dict:
    splits = jax.random.split(jax.random.key(seed), 6)
    return {
        "frames": centred(splits[0], (SEGMENT_COUNT, FRAMES, C), 1.0, 6.0, ((0, 128),)),
        "counts": plant(jax.random.randint(splits[1], (SEGMENT_COUNT,), 1, FRAMES + 1), jax.random.fold_in(splits[1], 1), 1, FRAMES).astype(jnp.int32),
        "positives": draw_positives(jax.random.fold_in(splits[5], 71), 0),
        "w_first": centred(splits[3], (C, H), C ** -0.5, 0.125, ((1, 16),)),
        "w_second": centred(splits[4], (H, E), H ** -0.5, 0.09375, ((0, 16),)),
    }


logit_sharpness_divisor = 0.05
score_top = 20.0

def reference(frames, counts, positives, w_first, w_second):
    frame_mask = (jnp.arange(FRAMES, dtype=jnp.int32)[None, :] < counts[:, None]).astype(jnp.float32)
    summed = jnp.einsum('rf,rfc->rc', frame_mask, frames.astype(jnp.float32))
    pooled = (summed / counts[:, None].astype(jnp.float32)).astype(jnp.bfloat16)
    preact = jnp.dot(pooled, w_first, preferred_element_type=jnp.float32)
    hidden = jax.nn.gelu(preact).astype(jnp.bfloat16)
    raw_keys = jnp.dot(hidden, w_second, preferred_element_type=jnp.float32)
    key_length = jnp.sqrt(lax.optimization_barrier(jnp.sum(raw_keys * raw_keys, axis=1, keepdims=True)) + 1e-06)
    unit_keys = raw_keys / key_length
    lower_match_vectors = unit_keys.astype(jnp.bfloat16)
    block_rows = GROUP_CLIPS
    block_count = SEGMENT_COUNT // block_rows
    all_ids = jnp.arange(SEGMENT_COUNT, dtype=jnp.int32)

    def block_scores(index):
        offset = (index * block_rows).astype(jnp.int32)
        lower_entry_span = lax.dynamic_slice_in_dim(lower_match_vectors, offset, block_rows, 0)
        cosine_logit_matrix = lax.dot_general(lower_entry_span, lower_match_vectors, (((1,), (1,)), ((), ())), preferred_element_type=jnp.float32) / logit_sharpness_divisor
        row_ids = offset + jnp.arange(block_rows, dtype=jnp.int32)
        partner = lax.dynamic_slice_in_dim(positives, offset, block_rows, 0)
        self_mask = all_ids[None, :] == row_ids[:, None]
        pair_mask = all_ids[None, :] == partner[:, None]
        return (lower_entry_span, cosine_logit_matrix, self_mask, pair_mask)

    def first_pass(index):
        lower_entry_span, cosine_logit_matrix, self_mask, pair_mask = block_scores(index)
        exp_terms = jnp.where(self_mask, 0.0, jnp.exp(cosine_logit_matrix - score_top))
        log_norm = jnp.log(lax.optimization_barrier(jnp.sum(exp_terms, axis=1))) + score_top
        pos_score = lax.optimization_barrier(jnp.sum(jnp.where(pair_mask, cosine_logit_matrix, 0.0), axis=1))
        return (log_norm, pos_score)
    log_norm, pos_score = lax.map(first_pass, jnp.arange(block_count, dtype=jnp.int32))
    log_norm = log_norm.reshape(SEGMENT_COUNT)
    pos_score = pos_score.reshape(SEGMENT_COUNT)
    batch_loss = jnp.sum(log_norm - pos_score) / SEGMENT_COUNT

    def second_pass(carry, index):
        lower_entry_span, cosine_logit_matrix, self_mask, pair_mask = block_scores(index)
        offset = (index * block_rows).astype(jnp.int32)
        row_norm = lax.dynamic_slice_in_dim(log_norm, offset, block_rows, 0)
        probs = jnp.where(self_mask, 0.0, jnp.exp(cosine_logit_matrix - row_norm[:, None]))
        weights = (probs - pair_mask.astype(jnp.float32)).astype(jnp.bfloat16)
        source_share = jnp.dot(weights, lower_match_vectors, preferred_element_type=jnp.float32)
        carry = carry + lax.dot_general(weights, lower_entry_span, (((0,), (0,)), ((), ())), preferred_element_type=jnp.float32)
        return (carry, source_share)
    target_share, source_share = lax.scan(second_pass, jnp.zeros((SEGMENT_COUNT, E), jnp.float32), jnp.arange(block_count, dtype=jnp.int32))
    source_share = source_share.reshape(SEGMENT_COUNT, E)
    sphere_projected_derivative = (source_share + target_share) / (SEGMENT_COUNT * logit_sharpness_divisor)
    raw_grad = ((sphere_projected_derivative - unit_keys * lax.optimization_barrier(jnp.sum(unit_keys * sphere_projected_derivative, axis=1, keepdims=True))) / key_length).astype(jnp.bfloat16)
    grad_second = lax.dot_general(hidden, raw_grad, (((0,), (0,)), ((), ())), preferred_element_type=jnp.float32)
    hidden_grad = lax.dot_general(raw_grad, w_second, (((1,), (1,)), ((), ())), preferred_element_type=jnp.float32)
    unused, backward = jax.vjp(jax.nn.gelu, preact)
    preact_grad = backward(hidden_grad)[0].astype(jnp.bfloat16)
    grad_first = lax.dot_general(pooled, preact_grad, (((0,), (0,)), ((), ())), preferred_element_type=jnp.float32)
    return (batch_loss, grad_first, grad_second)
```

```python
import jax
import jax.numpy as jnp
from jax import lax
from jax.sharding import Mesh
from jax.sharding import PartitionSpec as P

BLK = ("x", "zh")
GRP = ("zl", "y", "c")
ALL = ("x", "zh", "zl", "y", "c")
Z = ("zh", "zl")
XZ = ("x", "zh", "zl")


sharpness = 0.05
score_top = 20.0
bf16 = jnp.bfloat16
f32 = jnp.float32


def shift(block, axis, distance):
    n = lax.axis_size(axis)
    return lax.ppermute(block, axis, [(i, (i + distance) % n) for i in range(n)])


def swap(block):
    return lax.ppermute(block, "c", [(0, 1), (1, 0)])


def from_everyone(array, axis):
    peers = lax.axis_size(axis)
    return lax.all_to_all(
        jnp.broadcast_to(array[None], (peers, *array.shape)), axis, 0, 0, tiled=True
    )


def shards(frames, counts, positives, w_first, w_second):
    rows = frames.shape[0]
    slots = frames.shape[1]
    hid = w_first.shape[1]
    wide = w_second.shape[1]
    chan = w_first.shape[0]
    total = rows * 128
    x, zh, zl = lax.axis_index("x"), lax.axis_index("zh"), lax.axis_index("zl")
    y, c = lax.axis_index("y"), lax.axis_index("c")

    def first_row(xx, zzh, zzl, yy, cc):
        return ((((xx * 2 + zzh) * 2 + zzl) * 4 + yy) * 2 + cc) * rows

    half_c = chan // 2
    w1_far = jnp.concatenate(
        [shift(w_first[:half_c], Z, 1), shift(w_first[half_c:], Z, -1)], axis=0
    )
    w2_far = shift(w_second, Z, 1)
    w1_own = jnp.concatenate([w_first, w1_far], axis=1)
    w2_own = jnp.concatenate([w_second, w2_far], axis=0)
    w1_mate = swap(w1_own)
    w2_mate = swap(w2_own)
    w1_all = jnp.concatenate([w1_own, w1_mate], axis=1)
    w2_all = jnp.concatenate([w2_own, w2_mate], axis=0)

    mask = (jnp.arange(slots, dtype=jnp.int32)[None, :] < counts[:, None]).astype(bf16)
    summed = jnp.einsum("rf,rfc->rc", mask, frames, preferred_element_type=f32)
    pooled = (summed / counts[:, None].astype(f32)).astype(bf16)

    half_r = rows // 2
    from_prev = shift(pooled, "y", 1)
    from_next = shift(pooled, "y", -1)
    far_a = shift(from_prev[:half_r], "y", 1)
    far_b = shift(from_next[half_r:], "y", -1)
    near = jnp.concatenate([pooled, from_next, from_prev], axis=0)
    far = jnp.concatenate([far_a, far_b], axis=0)

    def forward(block):
        preact = jnp.dot(block, w1_all, preferred_element_type=f32)
        hidden = jax.nn.gelu(preact).astype(bf16)
        return preact, jnp.dot(hidden, w2_all, preferred_element_type=f32)

    pre_near, part_near = forward(near)
    pre_far, part_far = forward(far)
    raw_keys = (
        part_near[:rows]
        + shift(part_near[rows : 2 * rows], "y", 1)
        + shift(part_near[2 * rows :], "y", -1)
        + shift(part_far, "y", 2)
    )
    key_length = jnp.sqrt(jnp.sum(raw_keys * raw_keys, axis=1, keepdims=True) + 1e-06)
    unit = raw_keys / key_length
    unit_half = unit.astype(bf16)

    own_units = 2 * hid
    pre_rows = jnp.concatenate([pre_near, pre_far], axis=0)
    pre_mate = swap(pre_rows[:, own_units:])
    pool_rows = jnp.concatenate([near, far], axis=0)
    pool_mate = swap(pool_rows)
    pos_pair = jnp.stack([positives, swap(positives)])
    pos_rows = jnp.stack([pos_pair] + [shift(pos_pair, "y", -d) for d in (1, 2, 3)])

    pair = jnp.stack([unit_half, swap(unit_half)])
    tile_rows = jnp.stack([pair] + [shift(pair, "y", -d) for d in (1, 2, 3)])
    tile_rows = tile_rows.reshape(8 * rows, wide)
    tile_cols = from_everyone(unit_half, XZ).reshape(16 * rows, wide)

    local = jnp.arange(rows, dtype=jnp.int32)
    row_ids = jnp.stack(
        [
            jnp.stack([first_row(x, zh, zl, (y + d) % 4, cc) + local for cc in (c, 1 - c)])
            for d in range(4)
        ]
    ).reshape(8 * rows)
    col_ids = jnp.concatenate(
        [
            first_row(xx, zzh, zzl, y, c) + local
            for xx in range(4)
            for zzh in range(2)
            for zzl in range(2)
        ]
    )
    pos_ids = pos_rows.reshape(8 * rows)
    scores = (
        lax.dot_general(tile_rows, tile_cols, (((1,), (1,)), ((), ())), preferred_element_type=f32)
        / sharpness
    )
    self_mask = row_ids[:, None] == col_ids[None, :]
    pair_mask = pos_ids[:, None] == col_ids[None, :]
    exps = jnp.where(self_mask, 0.0, jnp.exp(scores - score_top))
    pos_part = jnp.sum(jnp.where(pair_mask, scores, 0.0))
    row_part = jnp.sum(exps, axis=1)
    col_part = jnp.sum(exps, axis=0)

    vec = jnp.concatenate(
        [row_part.reshape(8, rows), jnp.full((8, rows), pos_part, f32)], axis=0
    ).reshape(2, 4, 2, rows)
    got = [shift(vec, "y", d) for d in (1, 2, 3)]
    for d, piece in zip((1, 2, 3), got):
        vec = vec + jnp.roll(piece, -d, axis=1)
    vec = vec + jnp.flip(swap(vec), axis=2)
    row_sum = vec[0].reshape(8 * rows)
    col_sum = jnp.sum(from_everyone(col_part, XZ), axis=0)
    row_log = jnp.log(row_sum) + score_top
    loss_here = jnp.sum(row_log) - vec[1, 0, 0, 0]

    pair_float = pair_mask.astype(f32)
    weights = (exps * (1.0 / row_sum)[:, None] - pair_float).astype(bf16)
    mirror = (exps * (1.0 / col_sum)[None, :] - pair_float).astype(bf16)
    grad_part = jnp.dot(weights, tile_cols, preferred_element_type=f32) + jnp.dot(
        mirror, tile_cols, preferred_element_type=f32
    )
    grad_part = grad_part.reshape(4, 2, rows, wide)
    grad_core = grad_part[:, 0] + swap(grad_part[:, 1])
    unit_grad = (
        grad_core[0]
        + shift(grad_core[1], "y", 1)
        + shift(grad_core[2], "y", 2)
        + shift(grad_core[3], "y", 3)
    ) / (total * sharpness)
    raw_grad = (
        (unit_grad - unit * jnp.sum(unit * unit_grad, axis=1, keepdims=True)) / key_length
    ).astype(bf16)

    grad_pair = jnp.concatenate([raw_grad, swap(raw_grad)], axis=0)
    from_d = [grad_pair] + [shift(grad_pair, "y", -d) for d in (1, 2, 3)]
    order = (0, 1, 3, 2)
    grads = jnp.concatenate(
        [from_d[d][:rows] for d in order] + [from_d[d][rows:] for d in order], axis=0
    )
    pre_own = jnp.concatenate([pre_rows[:, :own_units], pre_mate], axis=0)
    pool_all = jnp.concatenate([pool_rows, pool_mate], axis=0)
    hidden_own, backward = jax.vjp(jax.nn.gelu, pre_own)
    second = lax.dot_general(
        hidden_own.astype(bf16), grads, (((0,), (0,)), ((), ())), preferred_element_type=f32
    )
    hidden_grad = lax.dot_general(
        grads, w2_own, (((1,), (1,)), ((), ())), preferred_element_type=f32
    )
    preact_grad = backward(hidden_grad)[0].astype(bf16)
    first = lax.dot_general(
        pool_all, preact_grad, (((0,), (0,)), ((), ())), preferred_element_type=f32
    )

    def parts(value):
        hi = value.astype(bf16).astype(f32)
        mid = (value - hi).astype(bf16).astype(f32)
        low = value - hi - mid
        return jnp.stack([hi, mid, low])

    term_far = jnp.concatenate([first[:, hid:], second[hid:]], axis=0).astype(bf16)
    term_own = jnp.concatenate([first[:, :hid], second[:hid]], axis=0)
    n_terms = chan + hid
    half_t = n_terms // 2
    add_a = shift(term_far[:half_t], Z, 1)
    add_b = shift(term_far[half_t:], Z, -1)
    loss_lane = jnp.pad(parts(loss_here), (0, 125)).astype(bf16)
    loss_far = shift(jnp.broadcast_to(loss_lane[None], (16, 128)), Z, 1)
    loss_two = loss_here + jnp.sum(loss_far[0].astype(f32))
    term_own = term_own + jnp.concatenate([add_a, add_b], axis=0).astype(f32)
    peers = 8
    piece = n_terms // peers
    extra = jnp.broadcast_to(
        jnp.pad(parts(loss_two), (0, wide - 3))[None, None], (peers, 16, wide)
    ).astype(bf16)
    sent = jnp.concatenate([term_own.astype(bf16).reshape(peers, piece, wide), extra], axis=1)
    got = lax.all_to_all(sent, BLK, 0, 0, tiled=True).astype(f32)
    mine = jnp.sum(got, axis=0)
    batch_loss = jnp.sum(mine[piece]) / total
    final = from_everyone(mine[:piece].astype(bf16), BLK).reshape(n_terms, wide).astype(f32)
    return (batch_loss, final[:chan], final[chan:])


def solution(mesh):
    finer = Mesh(mesh.devices.reshape(4, 2, 2, 4, 2), ALL)
    placed = (P(ALL, None, None), P(ALL), P(ALL), P(None, GRP), P(GRP, None))
    return jax.shard_map(
        shards,
        mesh=finer,
        in_specs=placed,
        out_specs=(P(), P(None, GRP), P(GRP, None)),
        check_vma=False,
    )
```

```python
import math

import jax
import jax.numpy as jnp
from jax import lax
from jax.experimental import pallas as pl
from jax.experimental.pallas import tpu as pltpu
from jax.sharding import Mesh
from jax.sharding import PartitionSpec as P


BLK = ("x", "zh")
GRP = ("zl", "y", "c")
ALL = ("x", "zh", "zl", "y", "c")
YC = ("y", "c")
ZC = ("zh", "zl", "c")
XZ = ("x", "zh", "zl")


bf16 = jnp.bfloat16
f32 = jnp.float32
i32 = jnp.int32

sharpness = 0.05
score_top = 20.0
log2e = math.log2(math.e)

ROWS = 128
HALF = 64
C = 2048
U = 256
E = 256
SLOTS = 8
TOTAL = 16384


def sds(shape, dtype):
    return jax.ShapeDtypeStruct(shape, dtype)


def kernel(body, outs, *args, grid=None, in_specs=None, out_specs=None, scratch=(), mib=24, flops=0):
    extra = {}
    if in_specs is not None:
        extra = dict(in_specs=in_specs, out_specs=out_specs)
    if grid is not None:
        extra["grid"] = grid
    return pl.pallas_call(
        body,
        out_shape=outs,
        scratch_shapes=list(scratch),
        compiler_params=pltpu.CompilerParams(vmem_limit_bytes=mib * 1024 * 1024),
        cost_estimate=pl.CostEstimate(flops=flops, bytes_accessed=0, transcendentals=0),
        **extra,
    )(*args)


def along_y(block, distance):
    return lax.ppermute(block, "y", [(i, (i + distance) % 4) for i in range(4)])


def swap(block):
    return lax.ppermute(block, "c", [(0, 1), (1, 0)])


def along_z(block):
    pairs = []
    for zz in range(4):
        pairs.append((zz * 2, ((zz + 1) % 4) * 2))
        pairs.append((zz * 2 + 1, ((zz - 1) % 4) * 2 + 1))
    return lax.ppermute(block, ZC, pairs)


def exchange(array, axis):
    return lax.all_to_all(array, axis, 0, 0, tiled=True)


def dot(a, b):
    return jnp.dot(a, b, preferred_element_type=f32)


def dot_t(a, b):
    return lax.dot_general(a, b, (((1,), (1,)), ((), ())), preferred_element_type=f32)


def join_weights(w1, w2, after, out):
    out[:C, :] = w1[...]
    out[C:, :] = w2[...]


def as_column(row):
    return jnp.broadcast_to(row, (ROWS, 128)).T


def pool_body(frames, counts, out_a, out_b, column):
    step = pl.program_id(0)

    @pl.when(step == 0)
    def _():
        column[...] = as_column(counts[...].astype(f32))

    n = column[pl.ds(pl.multiple_of(step * 32, 32), 32), 0:1]
    slot = lax.broadcasted_iota(i32, (32, 256), 1)
    row = lax.broadcasted_iota(i32, (32, 256), 0)
    low = row * SLOTS
    mask = ((slot >= low) & (slot < low + n.astype(i32))).astype(f32).astype(bf16)
    mean = (dot(mask, frames[...]) / n).astype(bf16)

    @pl.when(step < 2)
    def _():
        out_a[...] = mean

    @pl.when(step >= 2)
    def _():
        out_b[...] = mean


def gelu(v):
    k = math.sqrt(2.0 / math.pi)
    return v * (0.5 * (1.0 + jnp.tanh(k * (v + 0.044715 * (v * v * v)))))


def forward_sum(block, weights):
    total = None
    for w in weights:
        hidden = gelu(dot(block, w[:C, :])).astype(bf16)
        part = dot(hidden, w[C:, :])
        total = part if total is None else total + part
    return total


def near_body(a0, a1, a3, b0, b1, b3, own, far, mate, mate_far, near, p0, p1, p3):
    for i, piece in enumerate((a0, a1, a3, b0, b1, b3)):
        near[i * HALF : (i + 1) * HALF, :] = piece[...]
    part = forward_sum(near[...], (own, far, mate, mate_far))
    for i, out in enumerate((p0, p1, p3)):
        out[:HALF, :] = part[i * HALF : (i + 1) * HALF]
        out[HALF:, :] = part[(3 + i) * HALF : (4 + i) * HALF]


def far_body(a2, b2, own, far, mate, mate_far, block, p2):
    block[:HALF, :] = a2[...]
    block[HALF:, :] = b2[...]
    p2[...] = forward_sum(block[...], (own, far, mate, mate_far))


def keys_body(p0, p1, p2, p3, partner, raw, pay, spread):
    total = p0[...] + p1[...] + p2[...] + p3[...]
    raw[...] = total
    length = jnp.sqrt(jnp.sum(total * total, axis=1, keepdims=True) + 1e-06)
    half = (total / length).astype(bf16)
    row = partner[...]
    high = (row // 128).astype(f32)
    low = (row % 128).astype(f32)
    lane = lax.broadcasted_iota(i32, (ROWS, 128), 1)
    code = jnp.where(lane == 0, as_column(high), jnp.where(lane == 1, as_column(low), 0.0))
    code = code.astype(bf16)
    for i in range(16):
        spread[i] = half
    pay[:, :E] = half
    pay[:, E:] = code


def pair_body(own, mate, out):
    out[:ROWS, :] = own[...]
    out[ROWS:, :] = mate[...]


def pair_sum_body(own, mate, out):
    for d in range(4):
        for m in range(2):
            r = 2 * d + m
            other = 2 * d + 1 - m
            out[r : r + 1, :] = own[r : r + 1, :] + mate[other : other + 1, :]


def column_ids(base, j):
    lane = lax.broadcasted_iota(i32, (1, 256), 1)
    block = 2 * j + lane // 128
    return base + block * 1024 + lane % 128


def exp_block(scaled, exps, where, j):
    exps[...] = jnp.exp2(scaled * (log2e / sharpness) - score_top * log2e)

    @pl.when(where[2] == j)
    def _():
        row = where[0] + lax.broadcasted_iota(i32, (ROWS, 1), 0)
        same = column_ids(where[1], j) == row
        exps[:ROWS, :] = jnp.where(same, 0.0, exps[:ROWS, :])


def place_body(given, out):
    for i in range(5):
        out[i] = given[i]


def score_body(where, pay0, pay1, pay2, pay3, cols, row_out, col_out, tile, who, exps, acc):
    for d, pay in enumerate((pay0, pay1, pay2, pay3)):
        tile[d * 256 : (d + 1) * 256, :] = pay[:, :E]
        code = pay[:, E:].astype(f32)
        who[d * 256 : (d + 1) * 256, :] = code[:, 0:1] * 128.0 + code[:, 1:2]
    mates = who[...]
    found = jnp.zeros((1, 256), f32)
    for j in range(8):
        block = cols[2 * j : 2 * j + 2].reshape(256, E)
        scaled = dot_t(tile[...], block)
        ids = column_ids(where[1], j)
        exp_block(scaled, exps, where, j)
        hit = mates == ids.astype(f32)
        found = found + jnp.sum(jnp.where(hit, scaled, 0.0), axis=0, keepdims=True)
        here = exps[...]
        two = here[:, :128] + here[:, 128:]
        if j == 0:
            acc[...] = two
        else:
            acc[...] += two
        sums = jnp.sum(here, axis=0, keepdims=True)
        for i in range(16):
            col_out[i, :, j * 256 : (j + 1) * 256] = sums
    positive = jnp.sum(found) / sharpness
    for i in range(16):
        col_out[i, :, 2048:] = jnp.full((1, 128), positive, f32)
    for r in range(8):
        total = jnp.sum(acc[r * ROWS : (r + 1) * ROWS, :].T, axis=0, keepdims=True)
        row_out[r : r + 1, :] = total


def weight_body(
    where, tile, who, cols, sum0, sum1, sum2, sum3, col_sums, out, loss, scale, exps, acc
):
    sums = (sum0, sum1, sum2, sum3)
    for r in range(8):
        d, m = divmod(r, 2)
        total = None
        for s in range(4):
            at = (d - s) % 4 * 2 + m
            part = sums[s][at : at + 1, :]
            total = part if total is None else total + part
        scale[r * ROWS : (r + 1) * ROWS, :] = as_column(1.0 / total)
    mates = who[...]
    by_row = scale[:, 0:1]
    columns = col_sums[0]
    for i in range(1, 16):
        columns = columns + col_sums[i]
    logs = jnp.log(columns[:, :2048]) + score_top
    loss[...] = jnp.full((1, 128), jnp.sum(logs) - jnp.sum(columns[:, 2048:2049]), f32)
    for j in range(8):
        block = cols[2 * j : 2 * j + 2].reshape(256, E)
        scaled = dot_t(tile[...], block)
        ids = column_ids(where[1], j)
        exp_block(scaled, exps, where, j)
        here = exps[...]
        hit = (mates == ids.astype(f32)).astype(f32)
        by_col = 1.0 / columns[:, j * 256 : (j + 1) * 256]
        weights = (here * by_row - hit).astype(bf16)
        mirror = (here * by_col - hit).astype(bf16)
        part = dot(weights, block) + dot(mirror, block)
        if j == 0:
            acc[...] = part
        elif j < 7:
            acc[...] += part
        else:
            part = acc[...] + part
            for r in range(8):
                d, m = divmod(r, 2)
                at = (where[3] + d) % 4 * 2 + (where[4] + m) % 2
                out[pl.ds(at, 1)] = part[r * ROWS : (r + 1) * ROWS].reshape(1, ROWS, E)


def raw_grad_body(raw, got, out):
    total = raw[...]
    length = jnp.sqrt(jnp.sum(total * total, axis=1, keepdims=True) + 1e-06)
    unit = total / length
    grad = got[0]
    for i in range(1, 8):
        grad = grad + got[i]
    grad = grad / (TOTAL * sharpness)
    along = jnp.sum(unit * grad, axis=1, keepdims=True)
    out[...] = ((grad - unit * along) / length).astype(bf16)


def bundle_body(own, other, loss, out):
    out[:ROWS, :] = own[...]
    out[ROWS : 2 * ROWS, :] = other[...]
    value = loss[:, 0:1]
    high = value.astype(bf16).astype(f32)
    mid = (value - high).astype(bf16).astype(f32)
    low = value - high - mid
    lane = lax.broadcasted_iota(i32, (16, E), 1)
    rows = jnp.where(lane == 0, high, jnp.where(lane == 1, mid, jnp.where(lane == 2, low, 0.0)))
    out[2 * ROWS :, :] = rows.astype(bf16)


def slope_body(*refs):
    pools, w1 = refs[:8], refs[8]
    hidden, slope, joined = refs[9:]
    k = math.sqrt(2.0 / math.pi)
    low = 0
    for pool in pools:
        n = pool.shape[0]
        v = dot(pool[...], w1[...])
        t = jnp.tanh(k * (v + 0.044715 * (v * v * v)))
        hidden[:, low : low + n] = (v * (0.5 * (1.0 + t))).astype(bf16).T
        joined[low : low + n, :] = pool[...]
        slope[low : low + n, :] = 0.5 * (1.0 + t) + (0.5 * v) * (1.0 - t * t) * (
            k * (1.0 + 3 * 0.044715 * (v * v))
        )
        low += n


def head_body(*refs):
    pool, hidden, slope, w2, rings = refs[0], refs[1], refs[2], refs[3], refs[4:12]
    out, loss, grads, turned, second = refs[12:]
    step = pl.program_id(0)

    @pl.when(step == 0)
    def _():
        low = 0
        for core in range(2):
            ring = rings[core * 4 : core * 4 + 4]
            for z in range(2):
                near = [(d, h) for h in range(2) for d in (0, 1, 3)]
                for d, h in near + [(2, 0), (2, 1)]:
                    at = z * ROWS + h * HALF
                    grads[low : low + HALF, :] = ring[d][at : at + HALF, :]
                    low += HALF
        pre = (dot_t(grads[...], w2[...]) * slope[...]).astype(bf16)
        turned[...] = pre.T
        second[...] = dot(hidden[...], grads[...]).astype(bf16)
        total = jnp.zeros((1, E), f32)
        for ring in rings:
            total = total + ring[2 * ROWS : 2 * ROWS + 16, :].astype(f32)[0:1]
        loss[...] = jnp.full((1, 128), jnp.sum(total) / TOTAL, f32)

    out[0, :U, :] = dot(turned[...], pool[...]).astype(bf16)
    out[0, U:, :] = second[pl.ds(pl.multiple_of(step * 32, 32), 32), :]


def piece_body(got, out):
    total = got[0].astype(f32)
    for i in range(1, 8):
        total = total + got[i].astype(f32)
    first = total[:U, :].T.astype(bf16)
    second = total[U:, :].astype(bf16)
    for i in range(8):
        out[i, :U, :] = first
        out[i, U:, :] = second


def final_body(got, first, second):
    for i in range(2):
        first[i * 256 : (i + 1) * 256, :] = got[i, :U, :].astype(f32)
        second[i * 32 : (i + 1) * 32, :] = got[i, U:, :].astype(f32)


def step(frames, counts, positives, w_first, w_second):
    x, zh, zl = lax.axis_index("x"), lax.axis_index("zh"), lax.axis_index("zl")
    y, c = lax.axis_index("y"), lax.axis_index("c")
    base = (y * 2 + c) * ROWS
    cell = x * 4 + zh * 2 + zl
    where = jnp.stack([cell * 1024 + base, base, cell // 2, y, c]).astype(i32)
    vm = pl.BlockSpec()
    smem = pl.BlockSpec(memory_space=pltpu.SMEM)
    hbm = pl.BlockSpec(memory_space=pl.ANY)

    a0, b0 = kernel(
        pool_body,
        (sds((HALF, C), bf16), sds((HALF, C), bf16)),
        frames.reshape(ROWS * SLOTS, C),
        counts.reshape(1, ROWS),
        grid=(4,),
        in_specs=[
            pl.BlockSpec((256, C), lambda i: (i, 0)),
            pl.BlockSpec((1, ROWS), lambda i: (0, 0)),
        ],
        out_specs=[
            pl.BlockSpec((32, C), lambda i: (jnp.minimum(i, 1), 0)),
            pl.BlockSpec((32, C), lambda i: (jnp.maximum(i - 2, 0), 0)),
        ],
        scratch=[pltpu.VMEM((ROWS, 128), f32)],
        flops=10**8,
    )
    a3, b1 = along_y(a0, 1), along_y(b0, -1)
    b3, a1 = along_y(b0, 1), along_y(a0, -1)
    a2, b2 = along_y(a3, 1), along_y(b1, -1)

    w_own = kernel(
        join_weights, sds((C + U, E), bf16), w_first, w_second, a0,
        in_specs=[vm, vm, hbm], out_specs=vm,
    )
    w_far = along_z(w_own)
    w_mate = swap(w_own)
    w_mate_far = swap(w_far)
    weights = (w_own, w_far, w_mate, w_mate_far)

    key_part = sds((ROWS, E), f32)
    near, p0, p1, p3 = kernel(
        near_body,
        (sds((6 * HALF, C), bf16), key_part, key_part, key_part),
        a0, a1, a3, b0, b1, b3, *weights,
        flops=2 * 10**9,
    )
    q1, q3 = along_y(p1, 1), along_y(p3, -1)
    far, p2 = kernel(
        far_body, (sds((ROWS, C), bf16), key_part), a2, b2, *weights, flops=5 * 10**8
    )
    q2 = along_y(p2, 2)
    raw, pay, spread = kernel(
        keys_body,
        (key_part, sds((ROWS, E + 128), bf16), sds((16, ROWS, E), bf16)),
        p0, q1, q2, q3, positives.reshape(1, ROWS),
    )
    cols = exchange(spread, XZ)
    pair = kernel(pair_body, sds((2 * ROWS, E + 128), bf16), pay, swap(pay))
    pairs = [pair] + [along_y(pair, -d) for d in (1, 2, 3)]

    z_near, z_far = along_z(near), along_z(far)
    core = (near, far, z_near, z_far)
    pools = core + tuple(swap(p) for p in core)
    hidden, slope, joined = kernel(
        slope_body,
        (sds((U, 16 * ROWS), bf16), sds((16 * ROWS, U), f32), sds((16 * ROWS, C), bf16)),
        *pools, w_first,
        mib=36,
        flops=2 * 10**9,
    )

    where = kernel(place_body, sds((5,), i32), where, in_specs=[smem], out_specs=smem)
    row_sums, col_sums, tile, who = kernel(
        score_body,
        (
            sds((8, ROWS), f32),
            sds((16, 1, 2176), f32),
            sds((1024, E), bf16),
            sds((1024, 1), f32),
        ),
        where, *pairs, cols,
        in_specs=[smem] + [vm] * 5,
        out_specs=[vm, vm, vm, vm],
        scratch=[pltpu.VMEM((1024, 256), f32), pltpu.VMEM((1024, 128), f32)],
        flops=10**9,
    )
    col_sums = exchange(col_sums, XZ)
    row_sums = kernel(pair_sum_body, sds((8, ROWS), f32), row_sums, swap(row_sums))
    row_sums = [row_sums] + [along_y(row_sums, -d) for d in (1, 2, 3)]
    where = kernel(place_body, sds((5,), i32), where, in_specs=[smem], out_specs=smem)
    grads, loss = kernel(
        weight_body,
        (sds((8, ROWS, E), f32), sds((1, 128), f32)),
        where, tile, who, cols, *row_sums, col_sums,
        in_specs=[smem] + [vm] * 8,
        out_specs=[vm, vm],
        scratch=[
            pltpu.VMEM((1024, 128), f32),
            pltpu.VMEM((1024, 256), f32),
            pltpu.VMEM((1024, E), f32),
        ],
        flops=3 * 10**9,
    )
    mine = exchange(grads, YC)
    raw_grad = kernel(raw_grad_body, sds((ROWS, E), bf16), raw, mine)
    z_grad = along_z(raw_grad)
    ring0 = kernel(bundle_body, sds((2 * ROWS + 16, E), bf16), raw_grad, z_grad, loss)
    ring = [ring0] + [along_y(ring0, -d) for d in (1, 2, 3)]
    ring = ring + [swap(r) for r in ring]
    ring_spec = pl.BlockSpec((2 * ROWS + 16, E), lambda j: (0, 0))
    send, loss_all = kernel(
        head_body,
        (sds((8, U + 32, E), bf16), sds((1, 128), f32)),
        joined, hidden, slope, w_second, *ring,
        grid=(8,),
        in_specs=[
            pl.BlockSpec((16 * ROWS, 256), lambda j: (0, j)),
            pl.BlockSpec((U, 16 * ROWS), lambda j: (0, 0)),
            pl.BlockSpec((16 * ROWS, U), lambda j: (0, 0)),
            pl.BlockSpec((U, E), lambda j: (0, 0)),
        ]
        + [ring_spec] * 8,
        out_specs=[
            pl.BlockSpec((1, U + 32, E), lambda j: (j, 0, 0)),
            pl.BlockSpec((1, 128), lambda j: (0, 0)),
        ],
        scratch=[
            pltpu.VMEM((16 * ROWS, E), bf16),
            pltpu.VMEM((U, 16 * ROWS), bf16),
            pltpu.VMEM((U, E), bf16),
        ],
        flops=2 * 10**9,
    )
    got = exchange(send, BLK)
    piece = kernel(piece_body, sds((8, U + 32, E), bf16), got)
    whole = exchange(piece, BLK)
    first, second = kernel(
        final_body,
        (sds((C, U), f32), sds((U, E), f32)),
        whole,
        grid=(4,),
        in_specs=[pl.BlockSpec((2, U + 32, E), lambda j: (j, 0, 0))],
        out_specs=[
            pl.BlockSpec((512, U), lambda j: (j, 0)),
            pl.BlockSpec((64, E), lambda j: (j, 0)),
        ],
    )
    return (loss_all[0, 0], first, second)


def solution(mesh):
    finer = Mesh(mesh.devices.reshape(4, 2, 2, 4, 2), ALL)
    placed = (P(ALL, None, None), P(ALL), P(ALL), P(None, GRP), P(GRP, None))
    return jax.shard_map(
        step,
        mesh=finer,
        in_specs=placed,
        out_specs=(P(), P(None, GRP), P(GRP, None)),
        check_vma=False,
    )
```

```python
import math

import jax
import jax.numpy as jnp
from jax import lax
from jax.experimental import pallas as pl
from jax.experimental.pallas import tpu as pltpu
from jax.sharding import Mesh
from jax.sharding import PartitionSpec as P


BLK = ("x", "zh")
GRP = ("zl", "y", "c")
ALL = ("x", "zh", "zl", "y", "c")
ZC = ("zh", "zl", "c")
XZ = ("x", "zh", "zl")


bf16 = jnp.bfloat16
f32 = jnp.float32
i32 = jnp.int32

sharpness = 0.05
log2e = math.log2(math.e)

ROWS = 128
HALF = 64
C = 2048
U = 256
E = 256
SLOTS = 8
TOTAL = 16384
CELLS = (0, 1, 3, 2)


def sds(shape, dtype):
    return jax.ShapeDtypeStruct(shape, dtype)


def far_sds(shape, dtype):
    return pltpu.HBM(shape, dtype)


def kept(array):
    return pltpu.with_memory_space_constraint(array, pltpu.HBM)


def kernel(body, outs, *args, grid=None, in_specs=None, out_specs=None, scratch=(), mib=24, flops=0):
    extra = {}
    if in_specs is not None:
        extra = dict(in_specs=in_specs, out_specs=out_specs)
    if grid is not None:
        extra["grid"] = grid
    return pl.pallas_call(
        body,
        out_shape=outs,
        scratch_shapes=list(scratch),
        compiler_params=pltpu.CompilerParams(vmem_limit_bytes=mib * 1024 * 1024),
        cost_estimate=pl.CostEstimate(flops=flops, bytes_accessed=0, transcendentals=0),
        **extra,
    )(*args)


def along_y(block, distance):
    return lax.ppermute(block, "y", [(i, (i + distance) % 4) for i in range(4)])


def swap(block):
    return lax.ppermute(block, "c", [(0, 1), (1, 0)])


def along_z(block):
    pairs = []
    for zz in range(4):
        pairs.append((zz * 2, ((zz + 1) % 4) * 2))
        pairs.append((zz * 2 + 1, ((zz - 1) % 4) * 2 + 1))
    return lax.ppermute(block, ZC, pairs)


def exchange(array, axis):
    return lax.all_to_all(array, axis, 0, 0, tiled=True)


def dot(a, b):
    return jnp.dot(a, b, preferred_element_type=f32)


def dot_t(a, b):
    return lax.dot_general(a, b, (((1,), (1,)), ((), ())), preferred_element_type=f32)


def as_column(row):
    return jnp.broadcast_to(row, (ROWS, 128)).T


def pool_body(frames, counts, out_a, out_b, column):
    step = pl.program_id(0)

    @pl.when(step == 0)
    def _():
        column[...] = as_column(counts[...].astype(f32))

    slot = lax.broadcasted_iota(i32, (32, 256), 1)
    row = lax.broadcasted_iota(i32, (32, 256), 0)
    low = row * SLOTS

    def half(out):
        for i in range(2):
            at = pl.multiple_of(step * HALF + i * 32, 32)
            n = column[pl.ds(at, 32), 0:1]
            mask = ((slot >= low) & (slot < low + n.astype(i32))).astype(f32).astype(bf16)
            mean = dot(mask, frames[i * 256 : (i + 1) * 256, :]) / n
            out[i * 32 : (i + 1) * 32, :] = mean.astype(bf16)

    @pl.when(step == 0)
    def _():
        half(out_a)

    @pl.when(step == 1)
    def _():
        half(out_b)


def gelu(v):
    k = math.sqrt(2.0 / math.pi)
    return v * (0.5 * (1.0 + jnp.tanh(k * (v + 0.044715 * (v * v * v)))))


def forward_sum(block, weights):
    total = None
    for w1, w2 in zip(weights[:4], weights[4:]):
        hidden = gelu(dot(block, w1[...])).astype(bf16)
        part = dot(hidden, w2[...])
        total = part if total is None else total + part
    return total


def near_body(a0, b0, a1, b1, a3, b3, *refs):
    weights, (near, ring, p0, p1, p3) = refs[:8], refs[8:]
    for i, piece in enumerate((a0, b0, a1, b1, a3, b3)):
        near[i * HALF : (i + 1) * HALF, :] = piece[...]
    ring[...] = near[ROWS:, :]
    part = forward_sum(near[...], weights)
    for i, out in enumerate((p0, p1, p3)):
        out[...] = part[i * ROWS : (i + 1) * ROWS]


def far_body(a2, b2, *refs):
    weights, (block, p2) = refs[:8], refs[8:]
    block[:HALF, :] = a2[...]
    block[HALF:, :] = b2[...]
    p2[...] = forward_sum(block[...], weights)


def keys_body(p0, p1, p2, p3, partner, raw, pay, spread):
    total = p0[...] + p1[...] + p2[...] + p3[...]
    raw[...] = total
    length = jnp.sqrt(jnp.sum(total * total, axis=1, keepdims=True) + 1e-06)
    half = (total / length).astype(bf16)
    row = partner[...]
    high = (row // 128).astype(f32)
    low = (row % 128).astype(f32)
    lane = lax.broadcasted_iota(i32, (ROWS, 128), 1)
    code = jnp.where(lane == 0, as_column(high), jnp.where(lane == 1, as_column(low), 0.0))
    code = code.astype(bf16)
    for i in range(16):
        spread[i] = half
    pay[:, :E] = half
    pay[:, E:] = code


def pair_body(own, mate, out):
    out[:ROWS, :] = own[...]
    out[ROWS:, :] = mate[...]


def pair_sum_body(own, mate, out):
    for d in range(4):
        for m in range(2):
            r = 2 * d + m
            other = 2 * d + 1 - m
            out[r : r + 1, :] = own[r : r + 1, :] + mate[other : other + 1, :]


def column_ids(base, j):
    lane = lax.broadcasted_iota(i32, (1, 256), 1)
    block = 2 * j + lane // 128
    return base + block * 1024 + lane % 128


def exp_block(scaled, ids, own_row):
    exps = jnp.exp2(scaled * (log2e / sharpness))
    row = own_row + lax.broadcasted_iota(i32, (ROWS, 1), 0)
    return jnp.concatenate([jnp.where(ids == row, 0.0, exps[:ROWS]), exps[ROWS:]], axis=0)


def place_body(given, out):
    for i in range(5):
        out[i] = given[i]


def score_body(where, pay0, pay1, pay2, pay3, cols, row_out, col_out, tile, who, acc):
    for d, pay in enumerate((pay0, pay1, pay2, pay3)):
        tile[d * 256 : (d + 1) * 256, :] = pay[:, :E]
        code = pay[:, E:].astype(f32)
        number = code[:, 0:1] * 128.0 + code[:, 1:2]
        who[d * 256 : (d + 1) * 256, :] = jnp.broadcast_to(number, (256, 128))
    found = jnp.zeros((1, 256), f32)
    for j in range(8):
        block = cols[2 * j : 2 * j + 2].reshape(256, E)
        scaled = dot_t(tile[...], block)
        ids = column_ids(where[1], j)
        here = exp_block(scaled, ids, where[0])
        ids = ids.astype(f32)
        hit = jnp.concatenate([who[...] == ids[:, :128], who[...] == ids[:, 128:]], axis=1)
        found = found + jnp.sum(jnp.where(hit, scaled, 0.0), axis=0, keepdims=True)
        two = here[:, :128] + here[:, 128:]
        if j == 0:
            acc[...] = two
        else:
            acc[...] += two
        sums = jnp.sum(here, axis=0, keepdims=True)
        for i in range(16):
            col_out[i, :, j * 256 : (j + 1) * 256] = sums
    positive = jnp.sum(found) / sharpness
    for i in range(16):
        col_out[i, :, 2048:] = jnp.full((1, 128), positive, f32)
    for r in range(8):
        total = jnp.sum(acc[r * ROWS : (r + 1) * ROWS, :].T, axis=0, keepdims=True)
        row_out[r : r + 1, :] = total


def weight_body(
    where, tile, who, cols, sum0, sum1, sum2, sum3, col_sums, own, mate, loss, scale, acc
):
    sums = (sum0, sum1, sum2, sum3)
    for r in range(8):
        d, m = divmod(r, 2)
        total = None
        for s in range(4):
            at = (d - s) % 4 * 2 + m
            part = sums[s][at : at + 1, :]
            total = part if total is None else total + part
        scale[r * ROWS : (r + 1) * ROWS, :] = as_column(1.0 / total)
    columns = col_sums[0]
    for i in range(1, 16):
        columns = columns + col_sums[i]
    logs = jnp.log(columns[:, :2048])
    loss[...] = jnp.full((1, 128), jnp.sum(logs) - jnp.sum(columns[:, 2048:2049]), f32)
    for j in range(8):
        block = cols[2 * j : 2 * j + 2].reshape(256, E)
        scaled = dot_t(tile[...], block)
        ids = column_ids(where[1], j)
        here = exp_block(scaled, ids, where[0])
        ids = ids.astype(f32)
        by_col = 1.0 / columns[:, j * 256 : (j + 1) * 256]
        sides = [], []
        for low in (0, 128):
            half = here[:, low : low + 128]
            hit = jnp.where(who[...] == ids[:, low : low + 128], 1.0, 0.0)
            sides[0].append((half * scale[...] - hit).astype(bf16))
            sides[1].append((half * by_col[:, low : low + 128] - hit).astype(bf16))
        weights = jnp.concatenate(sides[0], axis=1)
        mirror = jnp.concatenate(sides[1], axis=1)
        part = dot(weights, block) + dot(mirror, block)
        if j == 0:
            acc[...] = part
        elif j < 7:
            acc[...] += part
        else:
            part = acc[...] + part
            for r in range(8):
                d, m = divmod(r, 2)
                out = mate if m else own
                out[pl.ds((where[3] + d) % 4, 1)] = part[r * ROWS : (r + 1) * ROWS].reshape(1, ROWS, E)


def add_body(a, b, out):
    out[...] = a[...] + b[...]


def raw_grad_body(raw, got, loss, out):
    total = raw[...]
    length = jnp.sqrt(jnp.sum(total * total, axis=1, keepdims=True) + 1e-06)
    unit = total / length
    grad = got[0]
    for i in range(1, 4):
        grad = grad + got[i]
    grad = grad / (TOTAL * sharpness)
    along = jnp.sum(unit * grad, axis=1, keepdims=True)
    out[:ROWS, :] = ((grad - unit * along) / length).astype(bf16)
    value = loss[:, 0:1]
    high = value.astype(bf16).astype(f32)
    mid = (value - high).astype(bf16).astype(f32)
    low = value - high - mid
    lane = lax.broadcasted_iota(i32, (16, E), 1)
    rows = jnp.where(lane == 0, high, jnp.where(lane == 1, mid, jnp.where(lane == 2, low, 0.0)))
    out[ROWS:, :] = rows.astype(bf16)


def slope_body(*refs):
    *pools, w1, hidden, slope, joined, acc = refs
    step = pl.program_id(0)
    low = 0
    for pool in pools:
        n = pool.shape[0]
        joined[low : low + n, :] = pool[...]
        low += n
    part = dot(joined[...], w1[...])

    @pl.when(step == 0)
    def _():
        acc[...] = part

    @pl.when(step > 0)
    def _():
        acc[...] += part

    @pl.when(step == 3)
    def _():
        k = math.sqrt(2.0 / math.pi)
        n = 256
        for low in range(0, 8 * ROWS, n):
            v = acc[low : low + n, :]
            t = jnp.tanh(k * (v + 0.044715 * (v * v * v)))
            hidden[:, low : low + n] = (v * (0.5 * (1.0 + t))).astype(bf16).T
            rise = k * (1.0 + 3 * 0.044715 * (v * v))
            turn = 0.5 * (1.0 + t) + (0.5 * v) * (1.0 - t * t) * rise
            slope[:, low : low + n] = turn.T


def head_body(pool_a, pool_b, hidden_a, hidden_b, slope_a, slope_b, w2, *refs):
    rings, (out, loss, grads, turned, second) = refs[:16], refs[16:]
    step = pl.program_id(0)
    rows = 8 * ROWS

    @pl.when(step == 0)
    def _():
        low = 0
        for z in range(2):
            for core in range(2):
                for d in CELLS:
                    grads[low : low + ROWS, :] = rings[z * 8 + core * 4 + d][:ROWS, :]
                    low += ROWS
        turned[:, :rows] = (dot_t(w2[...], grads[:rows, :]) * slope_a[...]).astype(bf16)
        turned[:, rows:] = (dot_t(w2[...], grads[rows:, :]) * slope_b[...]).astype(bf16)
        total = jnp.zeros((1, E), f32)
        for ring in rings[:8]:
            total = total + ring[ROWS : ROWS + 16, :].astype(f32)[0:1]
        loss[...] = jnp.full((1, 128), jnp.sum(total) / TOTAL, f32)
        both = dot(hidden_a[...], grads[:rows, :]) + dot(hidden_b[...], grads[rows:, :])
        second[...] = both.astype(bf16)

    first = dot(turned[:, :rows], pool_a[...]) + dot(turned[:, rows:], pool_b[...])
    first = first.astype(bf16)
    for i in range(2):
        out[i, :U, :] = first[:, i * 256 : (i + 1) * 256]
        out[i, U:, :] = second[pl.ds(pl.multiple_of(step * 64 + i * 32, 32), 32), :]


def piece_body(got, out):
    total = got[0].astype(f32)
    for i in range(1, 8):
        total = total + got[i].astype(f32)
    first = total[:U, :].T.astype(bf16)
    second = total[U:, :].astype(bf16)
    for i in range(8):
        out[i, :U, :] = first
        out[i, U:, :] = second


def final_body(got, first, second):
    for i in range(2):
        first[i * 256 : (i + 1) * 256, :] = got[i, :U, :].astype(f32)
        second[i * 32 : (i + 1) * 32, :] = got[i, U:, :].astype(f32)


def step(frames, counts, positives, w_first, w_second):
    x, zh, zl = lax.axis_index("x"), lax.axis_index("zh"), lax.axis_index("zl")
    y, c = lax.axis_index("y"), lax.axis_index("c")
    base = (y * 2 + c) * ROWS
    cell = x * 4 + zh * 2 + zl
    where = jnp.stack([cell * 1024 + base, base, cell // 2, y, c]).astype(i32)
    vm = pl.BlockSpec()
    smem = pl.BlockSpec(memory_space=pltpu.SMEM)
    hbm = pl.BlockSpec(memory_space=pl.ANY)

    w1_far = along_z(w_first)
    a0, b0 = kernel(
        pool_body,
        (sds((HALF, C), bf16), sds((HALF, C), bf16)),
        kept(frames.reshape(ROWS * SLOTS, C)),
        counts.reshape(1, ROWS),
        grid=(2,),
        in_specs=[
            pl.BlockSpec((512, C), lambda i: (i, 0)),
            pl.BlockSpec((1, ROWS), lambda i: (0, 0)),
        ],
        out_specs=[
            pl.BlockSpec((HALF, C), lambda i: (0, 0)),
            pl.BlockSpec((HALF, C), lambda i: (0, 0)),
        ],
        scratch=[pltpu.VMEM((ROWS, 128), f32)],
        flops=10**8,
    )
    a3, b1 = along_y(a0, 1), along_y(b0, -1)
    b3, a1 = along_y(b0, 1), along_y(a0, -1)
    a2, b2 = along_y(a3, 1), along_y(b1, -1)

    w1 = [w_first, w1_far, swap(w_first), swap(w1_far)]
    w2_far = along_z(w_second)
    w2 = [w_second, w2_far, swap(w_second), swap(w2_far)]
    weights = w1 + w2

    key_part = sds((ROWS, E), f32)
    near, near_ring, p0, p1, p3 = kernel(
        near_body,
        (far_sds((6 * HALF, C), bf16), far_sds((4 * HALF, C), bf16)) + (key_part,) * 3,
        a0, b0, a1, b1, a3, b3, *weights,
        flops=2 * 10**9,
    )
    q1, q3 = along_y(p1, 1), along_y(p3, -1)
    far, p2 = kernel(
        far_body, (far_sds((ROWS, C), bf16), key_part), a2, b2, *weights, flops=5 * 10**8
    )
    q2 = along_y(p2, 2)
    raw, pay, spread = kernel(
        keys_body,
        (far_sds((ROWS, E), f32), sds((ROWS, E + 128), bf16), far_sds((16, ROWS, E), bf16)),
        p0, q1, q2, q3, positives.reshape(1, ROWS),
    )
    cols = exchange(spread, XZ)
    pair = kernel(pair_body, sds((2 * ROWS, E + 128), bf16), pay, swap(pay))
    pairs = [pair] + [along_y(pair, -d) for d in (1, 2, 3)]

    own = (near, far)
    beside = (along_z(a0), along_z(b0), along_z(near_ring), along_z(far))

    def rows_of(pools):
        return kernel(
            slope_body,
            (
                far_sds((U, 8 * ROWS), bf16),
                far_sds((U, 8 * ROWS), f32),
                far_sds((8 * ROWS, C), bf16),
            ),
            *[kept(p) for p in pools], kept(w_first),
            grid=(4,),
            in_specs=[pl.BlockSpec((p.shape[0], 512), lambda j: (0, j)) for p in pools]
            + [pl.BlockSpec((512, U), lambda j: (j, 0))],
            out_specs=[
                pl.BlockSpec((U, 8 * ROWS), lambda j: (0, 0)),
                pl.BlockSpec((U, 8 * ROWS), lambda j: (0, 0)),
                pl.BlockSpec((8 * ROWS, 512), lambda j: (0, j)),
            ],
            scratch=[pltpu.VMEM((8 * ROWS, U), f32)],
            flops=2 * 10**9,
        )

    hidden_a, slope_a, joined_a = rows_of(own + (swap(near), swap(far)))
    hidden_b, slope_b, joined_b = rows_of(
        beside + tuple(swap(p) for p in beside[:3]) + (swap(beside[3]),)
    )

    where = kernel(
        place_body, sds((5,), i32), where, in_specs=[smem], out_specs=smem
    )
    row_sums, col_sums, tile, who = kernel(
        score_body,
        (
            sds((8, ROWS), f32),
            far_sds((16, 1, 2176), f32),
            far_sds((1024, E), bf16),
            far_sds((1024, 128), f32),
        ),
        where, *pairs, cols,
        in_specs=[smem] + [vm] * 5,
        out_specs=[vm, vm, vm, vm],
        scratch=[pltpu.VMEM((1024, 128), f32)],
        flops=10**9,
    )
    col_sums = exchange(col_sums, XZ)
    row_sums = kernel(pair_sum_body, sds((8, ROWS), f32), row_sums, swap(row_sums))
    row_sums = [row_sums] + [along_y(row_sums, -d) for d in (1, 2, 3)]
    where = kernel(
        place_body, sds((5,), i32), where, in_specs=[smem], out_specs=smem
    )
    grads, mate_grads, loss = kernel(
        weight_body,
        (
            sds((4, ROWS, E), f32),
            sds((4, ROWS, E), f32),
            far_sds((1, 128), f32),
        ),
        where, kept(tile), kept(who), kept(cols), *row_sums, col_sums,
        in_specs=[smem] + [vm] * 8,
        out_specs=[vm, vm, vm],
        scratch=[
            pltpu.VMEM((1024, 128), f32),
            pltpu.VMEM((1024, E), f32),
        ],
        flops=3 * 10**9,
    )
    grads = kernel(add_body, far_sds((4, ROWS, E), f32), grads, swap(mate_grads))
    mine = exchange(grads, "y")
    raw_grad = kernel(raw_grad_body, sds((ROWS + 16, E), bf16), kept(raw), mine, loss)
    z_grad = along_z(raw_grad)

    def ring_of(block):
        core = [block] + [along_y(block, -d) for d in (1, 2, 3)]
        return core + [swap(r) for r in core]

    ring = ring_of(raw_grad) + ring_of(z_grad)
    ring_spec = pl.BlockSpec((ROWS + 16, E), lambda j: (0, 0))
    send, loss_all = kernel(
        head_body,
        (sds((8, U + 32, E), bf16), sds((1, 128), f32)),
        kept(joined_a), kept(joined_b), hidden_a, hidden_b, slope_a, slope_b, kept(w_second), *ring,
        grid=(4,),
        in_specs=[
            pl.BlockSpec((8 * ROWS, 512), lambda j: (0, j)),
            pl.BlockSpec((8 * ROWS, 512), lambda j: (0, j)),
            pl.BlockSpec((U, 8 * ROWS), lambda j: (0, 0)),
            pl.BlockSpec((U, 8 * ROWS), lambda j: (0, 0)),
            pl.BlockSpec((U, 8 * ROWS), lambda j: (0, 0)),
            pl.BlockSpec((U, 8 * ROWS), lambda j: (0, 0)),
            pl.BlockSpec((U, E), lambda j: (0, 0)),
        ]
        + [ring_spec] * 16,
        out_specs=[
            pl.BlockSpec((2, U + 32, E), lambda j: (j, 0, 0)),
            pl.BlockSpec((1, 128), lambda j: (0, 0)),
        ],
        scratch=[
            pltpu.VMEM((16 * ROWS, E), bf16),
            pltpu.VMEM((U, 16 * ROWS), bf16),
            pltpu.VMEM((U, E), bf16),
        ],
        flops=2 * 10**9,
    )
    got = exchange(send, BLK)
    piece = kernel(piece_body, sds((8, U + 32, E), bf16), got)
    whole = exchange(piece, BLK)
    first, second = kernel(
        final_body,
        (sds((C, U), f32), sds((U, E), f32)),
        whole,
        grid=(4,),
        in_specs=[pl.BlockSpec((2, U + 32, E), lambda j: (j, 0, 0))],
        out_specs=[
            pl.BlockSpec((512, U), lambda j: (j, 0)),
            pl.BlockSpec((64, E), lambda j: (j, 0)),
        ],
    )
    return (loss_all[0, 0], first, second)


def solution(mesh):
    finer = Mesh(mesh.devices.reshape(4, 2, 2, 4, 2), ALL)
    placed = (P(ALL, None, None), P(ALL), P(ALL), P(None, GRP), P(GRP, None))
    return jax.shard_map(
        step,
        mesh=finer,
        in_specs=placed,
        out_specs=(P(), P(None, GRP), P(GRP, None)),
        check_vma=False,
    )
```

```python
import math

import jax
import jax.numpy as jnp
from jax import lax
from jax.experimental import pallas as pl
from jax.experimental.pallas import tpu as pltpu
from jax.sharding import Mesh
from jax.sharding import PartitionSpec as P


BLK = ("x", "zh")
GRP = ("zl", "y", "c")
ALL = ("x", "zh", "zl", "y", "c")
ZC = ("zh", "zl", "c")
XZ = ("x", "zh", "zl")


bf16 = jnp.bfloat16
f32 = jnp.float32
i32 = jnp.int32

sharpness = 0.05
log2e = math.log2(math.e)

ROWS = 128
HALF = 64
C = 2048
U = 256
E = 256
SLOTS = 8
TOTAL = 16384
CELLS = (0, 1, 3, 2)


def sds(shape, dtype):
    return jax.ShapeDtypeStruct(shape, dtype)


def far_sds(shape, dtype):
    return pltpu.HBM(shape, dtype)


def kept(array):
    return pltpu.with_memory_space_constraint(array, pltpu.HBM)


def kernel(body, outs, *args, grid=None, in_specs=None, out_specs=None, scratch=(), mib=24, flops=0):
    extra = {}
    if in_specs is not None:
        extra = dict(in_specs=in_specs, out_specs=out_specs)
    if grid is not None:
        extra["grid"] = grid
    return pl.pallas_call(
        body,
        out_shape=outs,
        scratch_shapes=list(scratch),
        compiler_params=pltpu.CompilerParams(vmem_limit_bytes=mib * 1024 * 1024),
        cost_estimate=pl.CostEstimate(flops=flops, bytes_accessed=0, transcendentals=0),
        **extra,
    )(*args)


def along_y(block, distance):
    return lax.ppermute(block, "y", [(i, (i + distance) % 4) for i in range(4)])


def swap(block):
    return lax.ppermute(block, "c", [(0, 1), (1, 0)])


def along_z(block):
    pairs = []
    for zz in range(4):
        pairs.append((zz * 2, ((zz + 1) % 4) * 2))
        pairs.append((zz * 2 + 1, ((zz - 1) % 4) * 2 + 1))
    return lax.ppermute(block, ZC, pairs)


def exchange(array, axis):
    return lax.all_to_all(array, axis, 0, 0, tiled=True)


def dot(a, b):
    return jnp.dot(a, b, preferred_element_type=f32)


def dot_t(a, b):
    return lax.dot_general(a, b, (((1,), (1,)), ((), ())), preferred_element_type=f32)


def as_column(row):
    return jnp.broadcast_to(row, (ROWS, 128)).T


def pool_body(frames, counts, out_a, out_b, column):
    step = pl.program_id(0)

    @pl.when(step == 0)
    def _():
        column[...] = as_column(counts[...].astype(f32))

    slot = lax.broadcasted_iota(i32, (32, 256), 1)
    row = lax.broadcasted_iota(i32, (32, 256), 0)
    low = row * SLOTS

    def half(out):
        for i in range(2):
            at = pl.multiple_of(step * HALF + i * 32, 32)
            n = column[pl.ds(at, 32), 0:1]
            mask = ((slot >= low) & (slot < low + n.astype(i32))).astype(f32).astype(bf16)
            mean = dot(mask, frames[i * 256 : (i + 1) * 256, :]) / n
            out[i * 32 : (i + 1) * 32, :] = mean.astype(bf16)

    @pl.when(step == 0)
    def _():
        half(out_a)

    @pl.when(step == 1)
    def _():
        half(out_b)


def gelu(v):
    k = math.sqrt(2.0 / math.pi)
    return v * (0.5 * (1.0 + jnp.tanh(k * (v + 0.044715 * (v * v * v)))))


def forward_sum(block, weights):
    total = None
    for w1, w2 in zip(weights[:4], weights[4:]):
        hidden = gelu(dot(block, w1[...])).astype(bf16)
        part = dot(hidden, w2[...])
        total = part if total is None else total + part
    return total


def near_body(a0, b0, a1, b1, a3, b3, *refs):
    weights, (near, ring, p0, p1, p3) = refs[:8], refs[8:]
    for i, piece in enumerate((a0, b0, a1, b1, a3, b3)):
        near[i * HALF : (i + 1) * HALF, :] = piece[...]
    ring[...] = near[ROWS:, :]
    part = forward_sum(near[...], weights)
    for i, out in enumerate((p0, p1, p3)):
        out[...] = part[i * ROWS : (i + 1) * ROWS]


def far_body(a2, b2, *refs):
    weights, (block, p2) = refs[:8], refs[8:]
    block[:HALF, :] = a2[...]
    block[HALF:, :] = b2[...]
    p2[...] = forward_sum(block[...], weights)


def keys_body(p0, p1, p2, p3, partner, raw, pay, spread):
    total = p0[...] + p1[...] + p2[...] + p3[...]
    raw[...] = total
    length = jnp.sqrt(jnp.sum(total * total, axis=1, keepdims=True) + 1e-06)
    half = (total / length).astype(bf16)
    row = partner[...]
    high = (row // 128).astype(f32)
    low = (row % 128).astype(f32)
    lane = lax.broadcasted_iota(i32, (ROWS, 128), 1)
    code = jnp.where(lane == 0, as_column(high), jnp.where(lane == 1, as_column(low), 0.0))
    code = code.astype(bf16)
    for i in range(16):
        spread[i] = half
    pay[:, :E] = half
    pay[:, E:] = code


def pair_body(own, mate, out):
    out[:ROWS, :] = own[...]
    out[ROWS:, :] = mate[...]


def pair_sum_body(own, mate, out):
    for d in range(4):
        for m in range(2):
            r = 2 * d + m
            other = 2 * d + 1 - m
            out[r : r + 1, :] = own[r : r + 1, :] + mate[other : other + 1, :]


def column_ids(base, j):
    lane = lax.broadcasted_iota(i32, (1, 256), 1)
    block = 2 * j + lane // 128
    return base + block * 1024 + lane % 128


def exp_block(scaled, ids, own_row):
    exps = jnp.exp2(scaled * (log2e / sharpness))
    row = own_row + lax.broadcasted_iota(i32, (ROWS, 1), 0)
    return jnp.concatenate([jnp.where(ids == row, 0.0, exps[:ROWS]), exps[ROWS:]], axis=0)


def score_body(where, pay0, pay1, pay2, pay3, cols, row_out, col_out, tile, who, acc):
    for d, pay in enumerate((pay0, pay1, pay2, pay3)):
        tile[d * 256 : (d + 1) * 256, :] = pay[:, :E]
        code = pay[:, E:].astype(f32)
        number = code[:, 0:1] * 128.0 + code[:, 1:2]
        who[d * 256 : (d + 1) * 256, :] = jnp.broadcast_to(number, (256, 128))
    found = jnp.zeros((1, 256), f32)
    for j in range(8):
        block = cols[2 * j : 2 * j + 2].reshape(256, E)
        scaled = dot_t(tile[...], block)
        ids = column_ids(where[1], j)
        here = exp_block(scaled, ids, where[0])
        ids = ids.astype(f32)
        hit = jnp.concatenate([who[...] == ids[:, :128], who[...] == ids[:, 128:]], axis=1)
        found = found + jnp.sum(jnp.where(hit, scaled, 0.0), axis=0, keepdims=True)
        two = here[:, :128] + here[:, 128:]
        if j == 0:
            acc[...] = two
        else:
            acc[...] += two
        sums = jnp.sum(here, axis=0, keepdims=True)
        for i in range(16):
            col_out[i, :, j * 256 : (j + 1) * 256] = sums
    positive = jnp.sum(found) / sharpness
    for i in range(16):
        col_out[i, :, 2048:] = jnp.full((1, 128), positive, f32)
    for r in range(8):
        total = jnp.sum(acc[r * ROWS : (r + 1) * ROWS, :].T, axis=0, keepdims=True)
        row_out[r : r + 1, :] = total


def scale_body(sum0, sum1, sum2, sum3, scale):
    sums = (sum0, sum1, sum2, sum3)
    for r in range(8):
        d, m = divmod(r, 2)
        total = None
        for s in range(4):
            at = (d - s) % 4 * 2 + m
            part = sums[s][at : at + 1, :]
            total = part if total is None else total + part
        scale[r * ROWS : (r + 1) * ROWS, :] = as_column(1.0 / total)


def weight_body(where, tile, who, cols, scale, col_sums, own, mate, loss, acc):
    columns = col_sums[0]
    for i in range(1, 16):
        columns = columns + col_sums[i]
    logs = jnp.log(columns[:, :2048])
    loss[...] = jnp.full((1, 128), jnp.sum(logs) - jnp.sum(columns[:, 2048:2049]), f32)
    for j in range(4):
        block = cols[4 * j : 4 * j + 4].reshape(512, E)
        sides = [], []
        for half in range(2):
            one = block[half * 256 : (half + 1) * 256]
            ids = column_ids(where[1], 2 * j + half)
            here = exp_block(dot_t(tile[...], one), ids, where[0])
            ids = ids.astype(f32)
            at = (2 * j + half) * 256
            by_col = 1.0 / columns[:, at : at + 256]
            for low in (0, 128):
                part = here[:, low : low + 128]
                hit = jnp.where(who[...] == ids[:, low : low + 128], 1.0, 0.0)
                sides[0].append((part * scale[...] - hit).astype(bf16))
                sides[1].append((part * by_col[:, low : low + 128] - hit).astype(bf16))
        both = jnp.concatenate(sides[0] + sides[1], axis=1)
        part = dot(both, jnp.concatenate([block, block], axis=0))
        if j == 0:
            acc[...] = part
        elif j < 3:
            acc[...] += part
        else:
            part = acc[...] + part
            for r in range(8):
                d, m = divmod(r, 2)
                out = mate if m else own
                out[pl.ds((where[3] + d) % 4, 1)] = part[r * ROWS : (r + 1) * ROWS].reshape(1, ROWS, E)


def add_body(a, b, out):
    out[...] = a[...] + b[...]


def raw_grad_body(raw, got, loss, out):
    total = raw[...]
    length = jnp.sqrt(jnp.sum(total * total, axis=1, keepdims=True) + 1e-06)
    unit = total / length
    grad = got[0]
    for i in range(1, 4):
        grad = grad + got[i]
    grad = grad / (TOTAL * sharpness)
    along = jnp.sum(unit * grad, axis=1, keepdims=True)
    out[:ROWS, :] = ((grad - unit * along) / length).astype(bf16)
    value = loss[:, 0:1]
    high = value.astype(bf16).astype(f32)
    mid = (value - high).astype(bf16).astype(f32)
    low = value - high - mid
    lane = lax.broadcasted_iota(i32, (16, E), 1)
    rows = jnp.where(lane == 0, high, jnp.where(lane == 1, mid, jnp.where(lane == 2, low, 0.0)))
    out[ROWS:, :] = rows.astype(bf16)


def slope_body(*refs):
    *pools, w1, hidden, slope, joined, acc = refs
    step = pl.program_id(0)
    low = 0
    for pool in pools:
        n = pool.shape[0]
        joined[low : low + n, :] = pool[...]
        low += n
    part = dot(joined[...], w1[...])

    @pl.when(step == 0)
    def _():
        acc[...] = part

    @pl.when(step > 0)
    def _():
        acc[...] += part

    @pl.when(step == 3)
    def _():
        k = math.sqrt(2.0 / math.pi)
        n = 256
        for low in range(0, 8 * ROWS, n):
            v = acc[low : low + n, :]
            t = jnp.tanh(k * (v + 0.044715 * (v * v * v)))
            hidden[:, low : low + n] = (v * (0.5 * (1.0 + t))).astype(bf16).T
            rise = k * (1.0 + 3 * 0.044715 * (v * v))
            turn = 0.5 * (1.0 + t) + (0.5 * v) * (1.0 - t * t) * rise
            slope[:, low : low + n] = turn.T


def head_body(pool_a, pool_b, hidden_a, hidden_b, slope_a, slope_b, w2, *refs):
    rings, (out, loss, grads, turned, second) = refs[:16], refs[16:]
    step = pl.program_id(0)
    rows = 8 * ROWS

    @pl.when(step == 0)
    def _():
        low = 0
        for z in range(2):
            for core in range(2):
                for d in CELLS:
                    grads[low : low + ROWS, :] = rings[z * 8 + core * 4 + d][:ROWS, :]
                    low += ROWS
        turned[:, :rows] = (dot_t(w2[...], grads[:rows, :]) * slope_a[...]).astype(bf16)
        turned[:, rows:] = (dot_t(w2[...], grads[rows:, :]) * slope_b[...]).astype(bf16)
        total = jnp.zeros((1, E), f32)
        for ring in rings[:8]:
            total = total + ring[ROWS : ROWS + 16, :].astype(f32)[0:1]
        loss[...] = jnp.full((1, 128), jnp.sum(total) / TOTAL, f32)
        both = dot(hidden_a[...], grads[:rows, :]) + dot(hidden_b[...], grads[rows:, :])
        second[...] = both.astype(bf16)

    first = dot(turned[:, :rows], pool_a[...]) + dot(turned[:, rows:], pool_b[...])
    first = first.astype(bf16)
    for i in range(2):
        out[i, :U, :] = first[:, i * 256 : (i + 1) * 256]
        out[i, U:, :] = second[pl.ds(pl.multiple_of(step * 64 + i * 32, 32), 32), :]


def piece_body(got, out):
    total = got[0].astype(f32)
    for i in range(1, 8):
        total = total + got[i].astype(f32)
    first = total[:U, :].T.astype(bf16)
    second = total[U:, :].astype(bf16)
    for i in range(8):
        out[i, :U, :] = first
        out[i, U:, :] = second


def final_body(got, first, second):
    for i in range(2):
        first[i * 256 : (i + 1) * 256, :] = got[i, :U, :].astype(f32)
        second[i * 32 : (i + 1) * 32, :] = got[i, U:, :].astype(f32)


def step(frames, counts, positives, w_first, w_second):
    x, zh, zl = lax.axis_index("x"), lax.axis_index("zh"), lax.axis_index("zl")
    y, c = lax.axis_index("y"), lax.axis_index("c")
    base = (y * 2 + c) * ROWS
    cell = x * 4 + zh * 2 + zl
    where = jnp.stack([cell * 1024 + base, base, cell // 2, y, c]).astype(i32)
    vm = pl.BlockSpec()
    smem = pl.BlockSpec(memory_space=pltpu.SMEM)
    hbm = pl.BlockSpec(memory_space=pl.ANY)

    w1_far = along_z(w_first)
    a0, b0 = kernel(
        pool_body,
        (sds((HALF, C), bf16), sds((HALF, C), bf16)),
        kept(frames.reshape(ROWS * SLOTS, C)),
        counts.reshape(1, ROWS),
        grid=(2,),
        in_specs=[
            pl.BlockSpec((512, C), lambda i: (i, 0)),
            pl.BlockSpec((1, ROWS), lambda i: (0, 0)),
        ],
        out_specs=[
            pl.BlockSpec((HALF, C), lambda i: (0, 0)),
            pl.BlockSpec((HALF, C), lambda i: (0, 0)),
        ],
        scratch=[pltpu.VMEM((ROWS, 128), f32)],
        flops=10**8,
    )
    a3, b1 = along_y(a0, 1), along_y(b0, -1)
    b3, a1 = along_y(b0, 1), along_y(a0, -1)
    a2, b2 = along_y(a3, 1), along_y(b1, -1)

    w1 = [w_first, w1_far, swap(w_first), swap(w1_far)]
    w2_far = along_z(w_second)
    w2 = [w_second, w2_far, swap(w_second), swap(w2_far)]
    weights = w1 + w2

    key_part = sds((ROWS, E), f32)
    near, near_ring, p0, p1, p3 = kernel(
        near_body,
        (far_sds((6 * HALF, C), bf16), far_sds((4 * HALF, C), bf16)) + (key_part,) * 3,
        a0, b0, a1, b1, a3, b3, *weights,
        flops=2 * 10**9,
    )
    q1, q3 = along_y(p1, 1), along_y(p3, -1)
    far, p2 = kernel(
        far_body, (far_sds((ROWS, C), bf16), key_part), a2, b2, *weights, flops=5 * 10**8
    )
    q2 = along_y(p2, 2)
    raw, pay, spread = kernel(
        keys_body,
        (far_sds((ROWS, E), f32), sds((ROWS, E + 128), bf16), far_sds((16, ROWS, E), bf16)),
        p0, q1, q2, q3, positives.reshape(1, ROWS),
    )
    cols = exchange(spread, XZ)
    pair = kernel(pair_body, sds((2 * ROWS, E + 128), bf16), pay, swap(pay))
    pairs = [pair] + [along_y(pair, -d) for d in (1, 2, 3)]

    own = (near, far)
    beside = (along_z(a0), along_z(b0), along_z(near_ring), along_z(far))

    def rows_of(pools):
        return kernel(
            slope_body,
            (
                far_sds((U, 8 * ROWS), bf16),
                far_sds((U, 8 * ROWS), f32),
                far_sds((8 * ROWS, C), bf16),
            ),
            *[kept(p) for p in pools], kept(w_first),
            grid=(4,),
            in_specs=[pl.BlockSpec((p.shape[0], 512), lambda j: (0, j)) for p in pools]
            + [pl.BlockSpec((512, U), lambda j: (j, 0))],
            out_specs=[
                pl.BlockSpec((U, 8 * ROWS), lambda j: (0, 0)),
                pl.BlockSpec((U, 8 * ROWS), lambda j: (0, 0)),
                pl.BlockSpec((8 * ROWS, 512), lambda j: (0, j)),
            ],
            scratch=[pltpu.VMEM((8 * ROWS, U), f32)],
            flops=2 * 10**9,
        )

    hidden_a, slope_a, joined_a = rows_of(own + (swap(near), swap(far)))
    hidden_b, slope_b, joined_b = rows_of(
        beside + tuple(swap(p) for p in beside[:3]) + (swap(beside[3]),)
    )

    row_sums, col_sums, tile, who = kernel(
        score_body,
        (
            sds((8, ROWS), f32),
            far_sds((16, 1, 2176), f32),
            far_sds((1024, E), bf16),
            far_sds((1024, 128), f32),
        ),
        where, *pairs, cols,
        in_specs=[smem] + [vm] * 5,
        out_specs=[vm, vm, vm, vm],
        scratch=[pltpu.VMEM((1024, 128), f32)],
        flops=10**9,
    )
    col_sums = exchange(col_sums, XZ)
    row_sums = kernel(pair_sum_body, sds((8, ROWS), f32), row_sums, swap(row_sums))
    row_sums = [row_sums] + [along_y(row_sums, -d) for d in (1, 2, 3)]
    scale = kernel(scale_body, sds((8 * ROWS, 128), f32), *row_sums)
    grads, mate_grads, loss = kernel(
        weight_body,
        (
            sds((4, ROWS, E), f32),
            sds((4, ROWS, E), f32),
            far_sds((1, 128), f32),
        ),
        where, kept(tile), kept(who), kept(cols), scale, col_sums,
        in_specs=[smem] + [vm] * 5,
        out_specs=[vm, vm, vm],
        scratch=[
            pltpu.VMEM((1024, E), f32),
        ],
        flops=3 * 10**9,
    )
    grads = kernel(add_body, far_sds((4, ROWS, E), f32), grads, swap(mate_grads))
    mine = exchange(grads, "y")
    raw_grad = kernel(raw_grad_body, sds((ROWS + 16, E), bf16), kept(raw), mine, loss)
    z_grad = along_z(raw_grad)

    def ring_of(block):
        core = [block] + [along_y(block, -d) for d in (1, 2, 3)]
        return core + [swap(r) for r in core]

    ring = ring_of(raw_grad) + ring_of(z_grad)
    ring_spec = pl.BlockSpec((ROWS + 16, E), lambda j: (0, 0))
    send, loss_all = kernel(
        head_body,
        (sds((8, U + 32, E), bf16), sds((1, 128), f32)),
        kept(joined_a), kept(joined_b), kept(hidden_a), kept(hidden_b), kept(slope_a), kept(slope_b), kept(w_second), *ring,
        grid=(4,),
        in_specs=[
            pl.BlockSpec((8 * ROWS, 512), lambda j: (0, j)),
            pl.BlockSpec((8 * ROWS, 512), lambda j: (0, j)),
            pl.BlockSpec((U, 8 * ROWS), lambda j: (0, 0)),
            pl.BlockSpec((U, 8 * ROWS), lambda j: (0, 0)),
            pl.BlockSpec((U, 8 * ROWS), lambda j: (0, 0)),
            pl.BlockSpec((U, 8 * ROWS), lambda j: (0, 0)),
            pl.BlockSpec((U, E), lambda j: (0, 0)),
        ]
        + [ring_spec] * 16,
        out_specs=[
            pl.BlockSpec((2, U + 32, E), lambda j: (j, 0, 0)),
            pl.BlockSpec((1, 128), lambda j: (0, 0)),
        ],
        scratch=[
            pltpu.VMEM((16 * ROWS, E), bf16),
            pltpu.VMEM((U, 16 * ROWS), bf16),
            pltpu.VMEM((U, E), bf16),
        ],
        flops=2 * 10**9,
    )
    got = exchange(send, BLK)
    piece = kernel(piece_body, sds((8, U + 32, E), bf16), got)
    whole = exchange(piece, BLK)
    first, second = kernel(
        final_body,
        (sds((C, U), f32), sds((U, E), f32)),
        whole,
        grid=(4,),
        in_specs=[pl.BlockSpec((2, U + 32, E), lambda j: (j, 0, 0))],
        out_specs=[
            pl.BlockSpec((512, U), lambda j: (j, 0)),
            pl.BlockSpec((64, E), lambda j: (j, 0)),
        ],
    )
    return (loss_all[0, 0], first, second)


def solution(mesh):
    finer = Mesh(mesh.devices.reshape(4, 2, 2, 4, 2), ALL)
    placed = (P(ALL, None, None), P(ALL), P(ALL), P(None, GRP), P(GRP, None))
    return jax.shard_map(
        step,
        mesh=finer,
        in_specs=placed,
        out_specs=(P(), P(None, GRP), P(GRP, None)),
        check_vma=False,
    )
```

```python
import math

import jax
import jax.numpy as jnp
from jax import lax
from jax.experimental import pallas as pl
from jax.experimental.pallas import tpu as pltpu
from jax.sharding import Mesh
from jax.sharding import PartitionSpec as P


BLK = ("x", "zh")
GRP = ("zl", "y", "c")
ALL = ("x", "zh", "zl", "y", "c")
ZC = ("zh", "zl", "c")
XZ = ("x", "zh", "zl")


bf16 = jnp.bfloat16
f32 = jnp.float32
i32 = jnp.int32

sharpness = 0.05
log2e = math.log2(math.e)

ROWS = 128
HALF = 64
C = 2048
U = 256
E = 256
SLOTS = 8
TOTAL = 16384
CELLS = (0, 1, 3, 2)


def sds(shape, dtype):
    return jax.ShapeDtypeStruct(shape, dtype)


def far_sds(shape, dtype):
    return pltpu.HBM(shape, dtype)


def kept(array):
    return pltpu.with_memory_space_constraint(array, pltpu.HBM)


def kernel(body, outs, *args, grid=None, in_specs=None, out_specs=None, scratch=(), mib=24, flops=0):
    extra = {}
    if in_specs is not None:
        extra = dict(in_specs=in_specs, out_specs=out_specs)
    if grid is not None:
        extra["grid"] = grid
    return pl.pallas_call(
        body,
        out_shape=outs,
        scratch_shapes=list(scratch),
        compiler_params=pltpu.CompilerParams(vmem_limit_bytes=mib * 1024 * 1024),
        cost_estimate=pl.CostEstimate(flops=flops, bytes_accessed=0, transcendentals=0),
        **extra,
    )(*args)


def along_y(block, distance):
    return lax.ppermute(block, "y", [(i, (i + distance) % 4) for i in range(4)])


def swap(block):
    return lax.ppermute(block, "c", [(0, 1), (1, 0)])


def along_z(block):
    pairs = []
    for zz in range(4):
        pairs.append((zz * 2, ((zz + 1) % 4) * 2))
        pairs.append((zz * 2 + 1, ((zz - 1) % 4) * 2 + 1))
    return lax.ppermute(block, ZC, pairs)


def exchange(array, axis):
    return lax.all_to_all(array, axis, 0, 0, tiled=True)


def dot(a, b):
    return jnp.dot(a, b, preferred_element_type=f32)


def dot_t(a, b):
    return lax.dot_general(a, b, (((1,), (1,)), ((), ())), preferred_element_type=f32)


def as_column(row):
    return jnp.broadcast_to(row, (ROWS, 128)).T


def pool_body(frames, counts, out_a, out_b, column):
    step = pl.program_id(0)

    @pl.when(step == 0)
    def _():
        column[...] = as_column(counts[...].astype(f32))

    slot = lax.broadcasted_iota(i32, (32, 256), 1)
    row = lax.broadcasted_iota(i32, (32, 256), 0)
    low = row * SLOTS

    def half(out):
        for i in range(2):
            at = pl.multiple_of(step * HALF + i * 32, 32)
            n = column[pl.ds(at, 32), 0:1]
            mask = ((slot >= low) & (slot < low + n.astype(i32))).astype(f32).astype(bf16)
            mean = dot(mask, frames[i * 256 : (i + 1) * 256, :]) / n
            out[i * 32 : (i + 1) * 32, :] = mean.astype(bf16)

    @pl.when(step == 0)
    def _():
        half(out_a)

    @pl.when(step == 1)
    def _():
        half(out_b)


def gelu(v):
    k = math.sqrt(2.0 / math.pi)
    return v * (0.5 * (1.0 + jnp.tanh(k * (v + 0.044715 * (v * v * v)))))


def forward_sum(block, weights):
    total = None
    for w1, w2 in zip(weights[:4], weights[4:]):
        hidden = gelu(dot(block, w1[...])).astype(bf16)
        part = dot(hidden, w2[...])
        total = part if total is None else total + part
    return total


def near_body(a0, b0, a1, b1, a3, b3, *refs):
    weights, (near, ring, p0, p1, p3) = refs[:8], refs[8:]
    for i, piece in enumerate((a0, b0, a1, b1, a3, b3)):
        near[i * HALF : (i + 1) * HALF, :] = piece[...]
    ring[...] = near[ROWS:, :]
    part = forward_sum(near[...], weights)
    for i, out in enumerate((p0, p1, p3)):
        out[...] = part[i * ROWS : (i + 1) * ROWS]


def far_body(a2, b2, *refs):
    weights, (block, p2) = refs[:8], refs[8:]
    block[:HALF, :] = a2[...]
    block[HALF:, :] = b2[...]
    p2[...] = forward_sum(block[...], weights)


def keys_body(p0, p1, p2, p3, partner, raw, pay, spread):
    total = p0[...] + p1[...] + p2[...] + p3[...]
    raw[...] = total
    length = jnp.sqrt(jnp.sum(total * total, axis=1, keepdims=True) + 1e-06)
    half = (total / length).astype(bf16)
    row = partner[...]
    high = (row // 128).astype(f32)
    low = (row % 128).astype(f32)
    lane = lax.broadcasted_iota(i32, (ROWS, 128), 1)
    code = jnp.where(lane == 0, as_column(high), jnp.where(lane == 1, as_column(low), 0.0))
    code = code.astype(bf16)
    for i in range(16):
        spread[i] = half
    pay[:, :E] = half
    pay[:, E:] = code


def pair_body(own, mate, out):
    out[:ROWS, :] = own[...]
    out[ROWS:, :] = mate[...]


def pair_sum_body(own, mate, out):
    for d in range(4):
        for m in range(2):
            r = 2 * d + m
            other = 2 * d + 1 - m
            out[r : r + 1, :] = own[r : r + 1, :] + mate[other : other + 1, :]


def column_ids(base, j):
    lane = lax.broadcasted_iota(i32, (1, 256), 1)
    block = 2 * j + lane // 128
    return base + block * 1024 + lane % 128


def exp_block(scaled, ids, own_row):
    exps = jnp.exp2(scaled * (log2e / sharpness))
    row = own_row + lax.broadcasted_iota(i32, (ROWS, 1), 0)
    return jnp.concatenate([jnp.where(ids == row, 0.0, exps[:ROWS]), exps[ROWS:]], axis=0)


def score_body(where, pay0, pay1, pay2, pay3, cols, row_out, col_out, tile, who, acc):
    for d, pay in enumerate((pay0, pay1, pay2, pay3)):
        tile[d * 256 : (d + 1) * 256, :] = pay[:, :E]
        code = pay[:, E:].astype(f32)
        number = code[:, 0:1] * 128.0 + code[:, 1:2]
        who[d * 256 : (d + 1) * 256, :] = jnp.broadcast_to(number, (256, 128))
    found = jnp.zeros((1, 256), f32)
    for j in range(8):
        block = cols[2 * j : 2 * j + 2].reshape(256, E)
        scaled = dot_t(tile[...], block)
        ids = column_ids(where[1], j)
        here = exp_block(scaled, ids, where[0])
        ids = ids.astype(f32)
        hit = jnp.concatenate([who[...] == ids[:, :128], who[...] == ids[:, 128:]], axis=1)
        found = found + jnp.sum(jnp.where(hit, scaled, 0.0), axis=0, keepdims=True)
        two = here[:, :128] + here[:, 128:]
        if j == 0:
            acc[...] = two
        else:
            acc[...] += two
        sums = jnp.sum(here, axis=0, keepdims=True)
        for i in range(16):
            col_out[i, :, j * 256 : (j + 1) * 256] = sums
    positive = jnp.sum(found) / sharpness
    for i in range(16):
        col_out[i, :, 2048:] = jnp.full((1, 128), positive, f32)
    for r in range(8):
        total = jnp.sum(acc[r * ROWS : (r + 1) * ROWS, :].T, axis=0, keepdims=True)
        row_out[r : r + 1, :] = total


def scale_body(sum0, sum1, sum2, sum3, scale):
    sums = (sum0, sum1, sum2, sum3)
    for r in range(8):
        d, m = divmod(r, 2)
        total = None
        for s in range(4):
            at = (d - s) % 4 * 2 + m
            part = sums[s][at : at + 1, :]
            total = part if total is None else total + part
        scale[r * ROWS : (r + 1) * ROWS, :] = as_column(1.0 / total)


def weight_body(where, tile, who, cols, scale, col_sums, own, mate, loss, acc):
    columns = col_sums[0]
    for i in range(1, 16):
        columns = columns + col_sums[i]
    logs = jnp.log(columns[:, :2048])
    loss[...] = jnp.full((1, 128), jnp.sum(logs) - jnp.sum(columns[:, 2048:2049]), f32)
    for j in range(4):
        block = cols[4 * j : 4 * j + 4].reshape(512, E)
        sides = [], []
        for half in range(2):
            one = block[half * 256 : (half + 1) * 256]
            ids = column_ids(where[1], 2 * j + half)
            here = exp_block(dot_t(tile[...], one), ids, where[0])
            ids = ids.astype(f32)
            at = (2 * j + half) * 256
            by_col = 1.0 / columns[:, at : at + 256]
            for low in (0, 128):
                part = here[:, low : low + 128]
                hit = jnp.where(who[...] == ids[:, low : low + 128], 1.0, 0.0)
                sides[0].append((part * scale[...] - hit).astype(bf16))
                sides[1].append((part * by_col[:, low : low + 128] - hit).astype(bf16))
        both = jnp.concatenate(sides[0] + sides[1], axis=1)
        part = dot(both, jnp.concatenate([block, block], axis=0))
        if j == 0:
            acc[...] = part
        elif j < 3:
            acc[...] += part
        else:
            part = acc[...] + part
            for r in range(8):
                d, m = divmod(r, 2)
                out = mate if m else own
                out[d] = part[r * ROWS : (r + 1) * ROWS]


def add_body(a, b, *outs):
    for d, out in enumerate(outs):
        out[...] = a[d] + b[d]


def raw_grad_body(raw, g0, g1, g2, g3, loss, out):
    total = raw[...]
    length = jnp.sqrt(jnp.sum(total * total, axis=1, keepdims=True) + 1e-06)
    unit = total / length
    grad = g0[...] + g1[...] + g2[...] + g3[...]
    grad = grad / (TOTAL * sharpness)
    along = jnp.sum(unit * grad, axis=1, keepdims=True)
    out[:ROWS, :] = ((grad - unit * along) / length).astype(bf16)
    value = loss[:, 0:1]
    high = value.astype(bf16).astype(f32)
    mid = (value - high).astype(bf16).astype(f32)
    low = value - high - mid
    lane = lax.broadcasted_iota(i32, (16, E), 1)
    rows = jnp.where(lane == 0, high, jnp.where(lane == 1, mid, jnp.where(lane == 2, low, 0.0)))
    out[ROWS:, :] = rows.astype(bf16)


def slope_body(*refs):
    *pools, w1, hidden, slope, joined, acc = refs
    step = pl.program_id(0)
    low = 0
    for pool in pools:
        n = pool.shape[0]
        joined[low : low + n, :] = pool[...]
        low += n
    part = dot(joined[...], w1[...])

    @pl.when(step == 0)
    def _():
        acc[...] = part

    @pl.when(step == 1)
    def _():
        k = math.sqrt(2.0 / math.pi)
        n = 256
        for low in range(0, 8 * ROWS, n):
            v = acc[low : low + n, :] + part[low : low + n, :]
            t = jnp.tanh(k * (v + 0.044715 * (v * v * v)))
            hidden[:, low : low + n] = (v * (0.5 * (1.0 + t))).astype(bf16).T
            rise = k * (1.0 + 3 * 0.044715 * (v * v))
            turn = 0.5 * (1.0 + t) + (0.5 * v) * (1.0 - t * t) * rise
            slope[:, low : low + n] = turn.T


def head_body(pool_a, pool_b, hidden_a, hidden_b, slope_a, slope_b, w2, *refs):
    rings, (out, loss, grads, turned, second) = refs[:16], refs[16:]
    step = pl.program_id(0)
    rows = 8 * ROWS

    @pl.when(step == 0)
    def _():
        low = 0
        for z in range(2):
            for core in range(2):
                for d in CELLS:
                    grads[low : low + ROWS, :] = rings[z * 8 + core * 4 + d][:ROWS, :]
                    low += ROWS
        turned[:, :rows] = (dot_t(w2[...], grads[:rows, :]) * slope_a[...]).astype(bf16)
        turned[:, rows:] = (dot_t(w2[...], grads[rows:, :]) * slope_b[...]).astype(bf16)
        total = jnp.zeros((1, E), f32)
        for ring in rings[:8]:
            total = total + ring[ROWS : ROWS + 16, :].astype(f32)[0:1]
        loss[...] = jnp.full((1, 128), jnp.sum(total) / TOTAL, f32)
        both = dot(hidden_a[...], grads[:rows, :]) + dot(hidden_b[...], grads[rows:, :])
        second[...] = both.astype(bf16)

    first = dot(turned[:, :rows], pool_a[...]) + dot(turned[:, rows:], pool_b[...])
    first = first.astype(bf16)
    for i in range(4):
        out[i, :U, :] = first[:, i * 256 : (i + 1) * 256]
        out[i, U:, :] = second[pl.ds(pl.multiple_of(step * 128 + i * 32, 32), 32), :]


def piece_body(got, out):
    total = got[0].astype(f32)
    for i in range(1, 8):
        total = total + got[i].astype(f32)
    first = total[:U, :].T.astype(bf16)
    second = total[U:, :].astype(bf16)
    for i in range(8):
        out[i, :U, :] = first
        out[i, U:, :] = second


def final_body(got, first, second):
    for i in range(4):
        first[i * 256 : (i + 1) * 256, :] = got[i, :U, :].astype(f32)
        second[i * 32 : (i + 1) * 32, :] = got[i, U:, :].astype(f32)


def step(frames, counts, positives, w_first, w_second):
    x, zh, zl = lax.axis_index("x"), lax.axis_index("zh"), lax.axis_index("zl")
    y, c = lax.axis_index("y"), lax.axis_index("c")
    base = (y * 2 + c) * ROWS
    cell = x * 4 + zh * 2 + zl
    where = jnp.stack([cell * 1024 + base, base, cell // 2, y, c]).astype(i32)
    vm = pl.BlockSpec()
    smem = pl.BlockSpec(memory_space=pltpu.SMEM)
    hbm = pl.BlockSpec(memory_space=pl.ANY)

    w1_far = along_z(w_first)
    a0, b0 = kernel(
        pool_body,
        (sds((HALF, C), bf16), sds((HALF, C), bf16)),
        kept(frames.reshape(ROWS * SLOTS, C)),
        counts.reshape(1, ROWS),
        grid=(2,),
        in_specs=[
            pl.BlockSpec((512, C), lambda i: (i, 0)),
            pl.BlockSpec((1, ROWS), lambda i: (0, 0)),
        ],
        out_specs=[
            pl.BlockSpec((HALF, C), lambda i: (0, 0)),
            pl.BlockSpec((HALF, C), lambda i: (0, 0)),
        ],
        scratch=[pltpu.VMEM((ROWS, 128), f32)],
        flops=10**8,
    )
    a3, b1 = along_y(a0, 1), along_y(b0, -1)
    b3, a1 = along_y(b0, 1), along_y(a0, -1)
    a2, b2 = along_y(a3, 1), along_y(b1, -1)

    w1 = [w_first, w1_far, swap(w_first), swap(w1_far)]
    w2_far = along_z(w_second)
    w2 = [w_second, w2_far, swap(w_second), swap(w2_far)]
    weights = w1 + w2

    key_part = sds((ROWS, E), f32)
    near, near_ring, p0, p1, p3 = kernel(
        near_body,
        (far_sds((6 * HALF, C), bf16), far_sds((4 * HALF, C), bf16)) + (key_part,) * 3,
        a0, b0, a1, b1, a3, b3, *weights,
        flops=2 * 10**9,
    )
    q1, q3 = along_y(p1, 1), along_y(p3, -1)
    far, p2 = kernel(
        far_body, (far_sds((ROWS, C), bf16), key_part), a2, b2, *weights, flops=5 * 10**8
    )
    q2 = along_y(p2, 2)
    raw, pay, spread = kernel(
        keys_body,
        (far_sds((ROWS, E), f32), sds((ROWS, E + 128), bf16), far_sds((16, ROWS, E), bf16)),
        p0, q1, q2, q3, positives.reshape(1, ROWS),
    )
    cols = exchange(spread, XZ)
    pair = kernel(pair_body, sds((2 * ROWS, E + 128), bf16), pay, swap(pay))
    pairs = [pair] + [along_y(pair, -d) for d in (1, 2, 3)]

    own = (near, far)
    beside = (along_z(a0), along_z(b0), along_z(near_ring), along_z(far))

    def rows_of(pools):
        return kernel(
            slope_body,
            (
                far_sds((U, 8 * ROWS), bf16),
                far_sds((U, 8 * ROWS), f32),
                far_sds((8 * ROWS, C), bf16),
            ),
            *[kept(p) for p in pools], kept(w_first),
            grid=(2,),
            in_specs=[pl.BlockSpec((p.shape[0], 1024), lambda j: (0, j)) for p in pools]
            + [pl.BlockSpec((1024, U), lambda j: (j, 0))],
            out_specs=[
                pl.BlockSpec((U, 8 * ROWS), lambda j: (0, 0)),
                pl.BlockSpec((U, 8 * ROWS), lambda j: (0, 0)),
                pl.BlockSpec((8 * ROWS, 1024), lambda j: (0, j)),
            ],
            scratch=[pltpu.VMEM((8 * ROWS, U), f32)],
            flops=2 * 10**9,
        )

    hidden_a, slope_a, joined_a = rows_of(own + (swap(near), swap(far)))
    hidden_b, slope_b, joined_b = rows_of(
        beside + tuple(swap(p) for p in beside[:3]) + (swap(beside[3]),)
    )

    row_sums, col_sums, tile, who = kernel(
        score_body,
        (
            sds((8, ROWS), f32),
            far_sds((16, 1, 2176), f32),
            far_sds((1024, E), bf16),
            far_sds((1024, 128), f32),
        ),
        where, *pairs, cols,
        in_specs=[smem] + [vm] * 5,
        out_specs=[vm, vm, vm, vm],
        scratch=[pltpu.VMEM((1024, 128), f32)],
        flops=10**9,
    )
    col_sums = exchange(col_sums, XZ)
    row_sums = kernel(pair_sum_body, sds((8, ROWS), f32), row_sums, swap(row_sums))
    row_sums = [row_sums] + [along_y(row_sums, -d) for d in (1, 2, 3)]
    scale = kernel(scale_body, sds((8 * ROWS, 128), f32), *row_sums)
    grads, mate_grads, loss = kernel(
        weight_body,
        (
            sds((4, ROWS, E), f32),
            sds((4, ROWS, E), f32),
            far_sds((1, 128), f32),
        ),
        where, kept(tile), kept(who), kept(cols), scale, col_sums,
        in_specs=[smem] + [vm] * 5,
        out_specs=[vm, vm, vm],
        scratch=[
            pltpu.VMEM((1024, E), f32),
        ],
        flops=3 * 10**9,
    )
    grads = kernel(add_body, (key_part,) * 4, grads, swap(mate_grads))
    mine = [grads[0]] + [along_y(grads[d], d) for d in (1, 2, 3)]
    raw_grad = kernel(raw_grad_body, sds((ROWS + 16, E), bf16), kept(raw), *mine, loss)
    ring = [raw_grad] + [along_y(raw_grad, -d) for d in (1, 2, 3)]
    zring = [along_z(raw_grad)] + [along_z(r) for r in ring[1:]]
    ring = ring + [swap(r) for r in ring]
    ring = ring + zring + [swap(r) for r in zring]
    ring_spec = pl.BlockSpec((ROWS + 16, E), lambda j: (0, 0))
    send, loss_all = kernel(
        head_body,
        (sds((8, U + 32, E), bf16), sds((1, 128), f32)),
        kept(joined_a), kept(joined_b), kept(hidden_a), kept(hidden_b), kept(slope_a), kept(slope_b), kept(w_second), *ring,
        grid=(2,),
        in_specs=[
            pl.BlockSpec((8 * ROWS, 1024), lambda j: (0, j)),
            pl.BlockSpec((8 * ROWS, 1024), lambda j: (0, j)),
            pl.BlockSpec((U, 8 * ROWS), lambda j: (0, 0)),
            pl.BlockSpec((U, 8 * ROWS), lambda j: (0, 0)),
            pl.BlockSpec((U, 8 * ROWS), lambda j: (0, 0)),
            pl.BlockSpec((U, 8 * ROWS), lambda j: (0, 0)),
            pl.BlockSpec((U, E), lambda j: (0, 0)),
        ]
        + [ring_spec] * 16,
        out_specs=[
            pl.BlockSpec((4, U + 32, E), lambda j: (j, 0, 0)),
            pl.BlockSpec((1, 128), lambda j: (0, 0)),
        ],
        scratch=[
            pltpu.VMEM((16 * ROWS, E), bf16),
            pltpu.VMEM((U, 16 * ROWS), bf16),
            pltpu.VMEM((U, E), bf16),
        ],
        flops=2 * 10**9,
    )
    got = exchange(send, BLK)
    piece = kernel(piece_body, sds((8, U + 32, E), bf16), got)
    whole = exchange(piece, BLK)
    first, second = kernel(
        final_body,
        (sds((C, U), f32), sds((U, E), f32)),
        whole,
        grid=(2,),
        in_specs=[pl.BlockSpec((4, U + 32, E), lambda j: (j, 0, 0))],
        out_specs=[
            pl.BlockSpec((1024, U), lambda j: (j, 0)),
            pl.BlockSpec((128, E), lambda j: (j, 0)),
        ],
    )
    return (loss_all[0, 0], first, second)


def solution(mesh):
    finer = Mesh(mesh.devices.reshape(4, 2, 2, 4, 2), ALL)
    placed = (P(ALL, None, None), P(ALL), P(ALL), P(None, GRP), P(GRP, None))
    return jax.shard_map(
        step,
        mesh=finer,
        in_specs=placed,
        out_specs=(P(), P(None, GRP), P(GRP, None)),
        check_vma=False,
    )
```

```python
import math

import jax
import jax.numpy as jnp
from jax import lax
from jax.experimental import pallas as pl
from jax.experimental.pallas import tpu as pltpu
from jax.sharding import Mesh
from jax.sharding import PartitionSpec as P


BLK = ("x", "zh")
GRP = ("zl", "y", "c")
ALL = ("x", "zh", "zl", "y", "c")
ZC = ("zh", "zl", "c")
XZ = ("x", "zh", "zl")


bf16 = jnp.bfloat16
f32 = jnp.float32
i32 = jnp.int32

sharpness = 0.05
log2e = math.log2(math.e)

ROWS = 128
HALF = 64
C = 2048
U = 256
E = 256
SLOTS = 8
TOTAL = 16384
CELLS = (0, 1, 3, 2)


def sds(shape, dtype):
    return jax.ShapeDtypeStruct(shape, dtype)


def far_sds(shape, dtype):
    return pltpu.HBM(shape, dtype)


def kept(array):
    return pltpu.with_memory_space_constraint(array, pltpu.HBM)


def kernel(body, outs, *args, grid=None, in_specs=None, out_specs=None, scratch=(), mib=24, flops=0):
    extra = {}
    if in_specs is not None:
        extra = dict(in_specs=in_specs, out_specs=out_specs)
    if grid is not None:
        extra["grid"] = grid
    return pl.pallas_call(
        body,
        out_shape=outs,
        scratch_shapes=list(scratch),
        compiler_params=pltpu.CompilerParams(vmem_limit_bytes=mib * 1024 * 1024),
        cost_estimate=pl.CostEstimate(flops=flops, bytes_accessed=0, transcendentals=0),
        **extra,
    )(*args)


def along_y(block, distance):
    return lax.ppermute(block, "y", [(i, (i + distance) % 4) for i in range(4)])


def swap(block):
    return lax.ppermute(block, "c", [(0, 1), (1, 0)])


def along_z(block):
    pairs = []
    for zz in range(4):
        pairs.append((zz * 2, ((zz + 1) % 4) * 2))
        pairs.append((zz * 2 + 1, ((zz - 1) % 4) * 2 + 1))
    return lax.ppermute(block, ZC, pairs)


def exchange(array, axis):
    return lax.all_to_all(array, axis, 0, 0, tiled=True)


def dot(a, b):
    return jnp.dot(a, b, preferred_element_type=f32)


def dot_t(a, b):
    return lax.dot_general(a, b, (((1,), (1,)), ((), ())), preferred_element_type=f32)


def as_column(row):
    return jnp.broadcast_to(row, (ROWS, 128)).T


def pool_body(frames, counts, out_a, out_b, column):
    step = pl.program_id(0)

    @pl.when(step == 0)
    def _():
        column[...] = as_column(counts[...].astype(f32))

    slot = lax.broadcasted_iota(i32, (32, 256), 1)
    row = lax.broadcasted_iota(i32, (32, 256), 0)
    low = row * SLOTS

    def half(out):
        for i in range(2):
            at = pl.multiple_of(step * HALF + i * 32, 32)
            n = column[pl.ds(at, 32), 0:1]
            mask = ((slot >= low) & (slot < low + n.astype(i32))).astype(f32).astype(bf16)
            mean = dot(mask, frames[i * 256 : (i + 1) * 256, :]) / n
            out[i * 32 : (i + 1) * 32, :] = mean.astype(bf16)

    @pl.when(step == 0)
    def _():
        half(out_a)

    @pl.when(step == 1)
    def _():
        half(out_b)


def gelu(v):
    k = math.sqrt(2.0 / math.pi)
    return v * (0.5 * (1.0 + jnp.tanh(k * (v + 0.044715 * (v * v * v)))))


def forward_sum(block, weights):
    total = None
    for w1, w2 in zip(weights[:4], weights[4:]):
        hidden = gelu(dot(block, w1[...])).astype(bf16)
        part = dot(hidden, w2[...])
        total = part if total is None else total + part
    return total


def near_body(a0, b0, a1, b1, a3, b3, *refs):
    weights, (near, ring, p0, p1, p3, acc) = refs[:8], refs[8:]
    step = pl.program_id(0)
    for i, piece in enumerate((a0, b0, a1, b1, a3, b3)):
        near[i * HALF : (i + 1) * HALF, :] = piece[...]
    ring[...] = near[ROWS:, :]
    parts = [dot(near[...], w1[...]) for w1 in weights[:4]]

    @pl.when(step == 0)
    def _():
        for i, part in enumerate(parts):
            acc[:, i * U : (i + 1) * U] = part

    @pl.when(step == 1)
    def _():
        total = None
        for i, part in enumerate(parts):
            hidden = gelu(acc[:, i * U : (i + 1) * U] + part).astype(bf16)
            keys = dot(hidden, weights[4 + i][...])
            total = keys if total is None else total + keys
        for i, out in enumerate((p0, p1, p3)):
            out[...] = total[i * ROWS : (i + 1) * ROWS]


def far_body(a2, b2, *refs):
    weights, (block, p2) = refs[:8], refs[8:]
    block[:HALF, :] = a2[...]
    block[HALF:, :] = b2[...]
    p2[...] = forward_sum(block[...], weights)


def keys_body(p0, p1, p2, p3, partner, raw, pay, spread):
    total = p0[...] + p1[...] + p2[...] + p3[...]
    raw[...] = total
    length = jnp.sqrt(jnp.sum(total * total, axis=1, keepdims=True) + 1e-06)
    half = (total / length).astype(bf16)
    row = partner[...]
    high = (row // 128).astype(f32)
    low = (row % 128).astype(f32)
    lane = lax.broadcasted_iota(i32, (ROWS, 128), 1)
    code = jnp.where(lane == 0, as_column(high), jnp.where(lane == 1, as_column(low), 0.0))
    code = code.astype(bf16)
    for i in range(16):
        spread[i] = half
    pay[:, :E] = half
    pay[:, E:] = code


def pair_body(own, mate, out):
    out[:ROWS, :] = own[...]
    out[ROWS:, :] = mate[...]


def pair_sum_body(own, mate, out):
    for d in range(4):
        for m in range(2):
            r = 2 * d + m
            other = 2 * d + 1 - m
            out[r : r + 1, :] = own[r : r + 1, :] + mate[other : other + 1, :]


def column_ids(base, j):
    lane = lax.broadcasted_iota(i32, (1, 256), 1)
    block = 2 * j + lane // 128
    return base + block * 1024 + lane % 128


def exp_block(scaled, ids, own_row):
    exps = jnp.exp2(scaled * (log2e / sharpness))
    row = own_row + lax.broadcasted_iota(i32, (ROWS, 1), 0)
    return jnp.concatenate([jnp.where(ids == row, 0.0, exps[:ROWS]), exps[ROWS:]], axis=0)


def score_body(where, pay0, pay1, pay2, pay3, cols, row_out, col_out, tile, who, acc):
    for d, pay in enumerate((pay0, pay1, pay2, pay3)):
        tile[d * 256 : (d + 1) * 256, :] = pay[:, :E]
        code = pay[:, E:].astype(f32)
        number = code[:, 0:1] * 128.0 + code[:, 1:2]
        who[d * 256 : (d + 1) * 256, :] = jnp.broadcast_to(number, (256, 128))
    found = jnp.zeros((1, 256), f32)
    for j in range(8):
        block = cols[2 * j : 2 * j + 2].reshape(256, E)
        scaled = dot_t(tile[...], block)
        ids = column_ids(where[1], j)
        here = exp_block(scaled, ids, where[0])
        ids = ids.astype(f32)
        hit = jnp.concatenate([who[...] == ids[:, :128], who[...] == ids[:, 128:]], axis=1)
        found = found + jnp.sum(jnp.where(hit, scaled, 0.0), axis=0, keepdims=True)
        two = here[:, :128] + here[:, 128:]
        if j == 0:
            acc[...] = two
        else:
            acc[...] += two
        sums = jnp.sum(here, axis=0, keepdims=True)
        for i in range(16):
            col_out[i, :, j * 256 : (j + 1) * 256] = sums
    positive = jnp.sum(found) / sharpness
    for i in range(16):
        col_out[i, :, 2048:] = jnp.full((1, 128), positive, f32)
    for r in range(8):
        total = jnp.sum(acc[r * ROWS : (r + 1) * ROWS, :].T, axis=0, keepdims=True)
        row_out[r : r + 1, :] = total


def scale_body(sum0, sum1, sum2, sum3, scale):
    sums = (sum0, sum1, sum2, sum3)
    for r in range(8):
        d, m = divmod(r, 2)
        total = None
        for s in range(4):
            at = (d - s) % 4 * 2 + m
            part = sums[s][at : at + 1, :]
            total = part if total is None else total + part
        scale[r * ROWS : (r + 1) * ROWS, :] = as_column(1.0 / total)


def weight_body(where, tile, who, cols, scale, col_sums, own, mate, loss, acc):
    columns = col_sums[0]
    for i in range(1, 16):
        columns = columns + col_sums[i]
    logs = jnp.log(columns[:, :2048])
    loss[...] = jnp.full((1, 128), jnp.sum(logs) - jnp.sum(columns[:, 2048:2049]), f32)
    for j in range(4):
        block = cols[4 * j : 4 * j + 4].reshape(512, E)
        sides = [], []
        for half in range(2):
            one = block[half * 256 : (half + 1) * 256]
            ids = column_ids(where[1], 2 * j + half)
            here = exp_block(dot_t(tile[...], one), ids, where[0])
            ids = ids.astype(f32)
            at = (2 * j + half) * 256
            by_col = 1.0 / columns[:, at : at + 256]
            for low in (0, 128):
                part = here[:, low : low + 128]
                hit = jnp.where(who[...] == ids[:, low : low + 128], 1.0, 0.0)
                sides[0].append((part * scale[...] - hit).astype(bf16))
                sides[1].append((part * by_col[:, low : low + 128] - hit).astype(bf16))
        both = jnp.concatenate(sides[0] + sides[1], axis=1)
        part = dot(both, jnp.concatenate([block, block], axis=0))
        if j == 0:
            acc[...] = part
        elif j < 3:
            acc[...] += part
        else:
            part = acc[...] + part
            for r in range(8):
                d, m = divmod(r, 2)
                out = mate if m else own
                out[d] = part[r * ROWS : (r + 1) * ROWS]


def add_body(a, b, *outs):
    for d, out in enumerate(outs):
        out[...] = a[d] + b[d]


def raw_grad_body(raw, g0, g1, g2, g3, loss, out):
    total = raw[...]
    length = jnp.sqrt(jnp.sum(total * total, axis=1, keepdims=True) + 1e-06)
    unit = total / length
    grad = g0[...] + g1[...] + g2[...] + g3[...]
    grad = grad / (TOTAL * sharpness)
    along = jnp.sum(unit * grad, axis=1, keepdims=True)
    out[:ROWS, :] = ((grad - unit * along) / length).astype(bf16)
    value = loss[:, 0:1]
    high = value.astype(bf16).astype(f32)
    mid = (value - high).astype(bf16).astype(f32)
    low = value - high - mid
    lane = lax.broadcasted_iota(i32, (16, E), 1)
    rows = jnp.where(lane == 0, high, jnp.where(lane == 1, mid, jnp.where(lane == 2, low, 0.0)))
    out[ROWS:, :] = rows.astype(bf16)


def slope_body(*refs):
    *pools, w1, hidden, slope, joined, acc = refs
    step = pl.program_id(0)
    low = 0
    for pool in pools:
        n = pool.shape[0]
        joined[low : low + n, :] = pool[...]
        low += n
    part = dot(joined[...], w1[...])

    @pl.when(step == 0)
    def _():
        acc[...] = part

    @pl.when(step == 1)
    def _():
        k = math.sqrt(2.0 / math.pi)
        n = 256
        for low in range(0, 8 * ROWS, n):
            v = acc[low : low + n, :] + part[low : low + n, :]
            t = jnp.tanh(k * (v + 0.044715 * (v * v * v)))
            hidden[:, low : low + n] = (v * (0.5 * (1.0 + t))).astype(bf16).T
            rise = k * (1.0 + 3 * 0.044715 * (v * v))
            turn = 0.5 * (1.0 + t) + (0.5 * v) * (1.0 - t * t) * rise
            slope[:, low : low + n] = turn.T


def head_body(pool_a, pool_b, hidden_a, hidden_b, slope_a, slope_b, w2, *refs):
    rings, (out, loss, grads, turned, second) = refs[:16], refs[16:]
    step = pl.program_id(0)
    rows = 8 * ROWS

    @pl.when(step == 0)
    def _():
        low = 0
        for z in range(2):
            for core in range(2):
                for d in CELLS:
                    grads[low : low + ROWS, :] = rings[z * 8 + core * 4 + d][:ROWS, :]
                    low += ROWS
        turned[:, :rows] = (dot_t(w2[...], grads[:rows, :]) * slope_a[...]).astype(bf16)
        turned[:, rows:] = (dot_t(w2[...], grads[rows:, :]) * slope_b[...]).astype(bf16)
        total = jnp.zeros((1, E), f32)
        for ring in rings[:8]:
            total = total + ring[ROWS : ROWS + 16, :].astype(f32)[0:1]
        loss[...] = jnp.full((1, 128), jnp.sum(total) / TOTAL, f32)
        both = dot(hidden_a[...], grads[:rows, :]) + dot(hidden_b[...], grads[rows:, :])
        second[...] = both.astype(bf16)

    first = dot(turned[:, :rows], pool_a[...]) + dot(turned[:, rows:], pool_b[...])
    first = first.astype(bf16)
    for i in range(4):
        out[i, :U, :] = first[:, i * 256 : (i + 1) * 256]
        out[i, U:, :] = second[pl.ds(pl.multiple_of(step * 128 + i * 32, 32), 32), :]


def piece_body(got, out):
    total = got[0].astype(f32)
    for i in range(1, 8):
        total = total + got[i].astype(f32)
    first = total[:U, :].T.astype(bf16)
    second = total[U:, :].astype(bf16)
    for i in range(8):
        out[i, :U, :] = first
        out[i, U:, :] = second


def final_body(got, first, second):
    for i in range(4):
        first[i * 256 : (i + 1) * 256, :] = got[i, :U, :].astype(f32)
        second[i * 32 : (i + 1) * 32, :] = got[i, U:, :].astype(f32)


def step(frames, counts, positives, w_first, w_second):
    x, zh, zl = lax.axis_index("x"), lax.axis_index("zh"), lax.axis_index("zl")
    y, c = lax.axis_index("y"), lax.axis_index("c")
    base = (y * 2 + c) * ROWS
    cell = x * 4 + zh * 2 + zl
    where = jnp.stack([cell * 1024 + base, base, cell // 2, y, c]).astype(i32)
    vm = pl.BlockSpec()
    smem = pl.BlockSpec(memory_space=pltpu.SMEM)
    hbm = pl.BlockSpec(memory_space=pl.ANY)

    w1_far = along_z(w_first)
    a0, b0 = kernel(
        pool_body,
        (sds((HALF, C), bf16), sds((HALF, C), bf16)),
        kept(frames.reshape(ROWS * SLOTS, C)),
        counts.reshape(1, ROWS),
        grid=(2,),
        in_specs=[
            pl.BlockSpec((512, C), lambda i: (i, 0)),
            pl.BlockSpec((1, ROWS), lambda i: (0, 0)),
        ],
        out_specs=[
            pl.BlockSpec((HALF, C), lambda i: (0, 0)),
            pl.BlockSpec((HALF, C), lambda i: (0, 0)),
        ],
        scratch=[pltpu.VMEM((ROWS, 128), f32)],
        flops=10**8,
    )
    a3, b1 = along_y(a0, 1), along_y(b0, -1)
    b3, a1 = along_y(b0, 1), along_y(a0, -1)
    a2, b2 = along_y(a3, 1), along_y(b1, -1)

    w1 = [w_first, w1_far, swap(w_first), swap(w1_far)]
    w2_far = along_z(w_second)
    w2 = [w_second, w2_far, swap(w_second), swap(w2_far)]
    weights = w1 + w2

    key_part = sds((ROWS, E), f32)
    near, near_ring, p0, p1, p3 = kernel(
        near_body,
        (far_sds((6 * HALF, C), bf16), far_sds((4 * HALF, C), bf16)) + (key_part,) * 3,
        a0, b0, a1, b1, a3, b3, *weights,
        grid=(2,),
        in_specs=[pl.BlockSpec((HALF, C // 2), lambda j: (0, j))] * 6
        + [pl.BlockSpec((C // 2, U), lambda j: (j, 0))] * 4
        + [pl.BlockSpec((U, E), lambda j: (0, 0))] * 4,
        out_specs=[
            pl.BlockSpec((6 * HALF, C // 2), lambda j: (0, j)),
            pl.BlockSpec((4 * HALF, C // 2), lambda j: (0, j)),
        ]
        + [pl.BlockSpec((ROWS, E), lambda j: (0, 0))] * 3,
        scratch=[pltpu.VMEM((6 * HALF, 4 * U), f32)],
        flops=2 * 10**9,
    )
    q1, q3 = along_y(p1, 1), along_y(p3, -1)
    far, p2 = kernel(
        far_body, (far_sds((ROWS, C), bf16), key_part), a2, b2, *weights, flops=5 * 10**8
    )
    q2 = along_y(p2, 2)
    raw, pay, spread = kernel(
        keys_body,
        (far_sds((ROWS, E), f32), sds((ROWS, E + 128), bf16), far_sds((16, ROWS, E), bf16)),
        p0, q1, q2, q3, positives.reshape(1, ROWS),
    )
    cols = exchange(spread, XZ)
    pair = kernel(pair_body, sds((2 * ROWS, E + 128), bf16), pay, swap(pay))
    pairs = [pair] + [along_y(pair, -d) for d in (1, 2, 3)]

    own = (near, far)
    beside = (along_z(a0), along_z(b0), along_z(near_ring), along_z(far))

    def rows_of(name, pools):
        return kernel(
            slope_body,
            (
                far_sds((U, 8 * ROWS), bf16),
                far_sds((U, 8 * ROWS), f32),
                far_sds((8 * ROWS, C), bf16),
            ),
            *(pools if name == "slopez" else [kept(p) for p in pools]), kept(w_first),
            grid=(2,),
            in_specs=[pl.BlockSpec((p.shape[0], 1024), lambda j: (0, j)) for p in pools]
            + [pl.BlockSpec((1024, U), lambda j: (j, 0))],
            out_specs=[
                pl.BlockSpec((U, 8 * ROWS), lambda j: (0, 0)),
                pl.BlockSpec((U, 8 * ROWS), lambda j: (0, 0)),
                pl.BlockSpec((8 * ROWS, 1024), lambda j: (0, j)),
            ],
            scratch=[pltpu.VMEM((8 * ROWS, U), f32)],
            flops=2 * 10**9,
        )

    hidden_a, slope_a, joined_a = rows_of("slope", own + (swap(near), swap(far)))
    hidden_b, slope_b, joined_b = rows_of(
        "slopez",
        beside
        + tuple(swap(p) for p in beside[:3])
        + (swap(beside[3]),),
    )

    row_sums, col_sums, tile, who = kernel(
        score_body,
        (
            sds((8, ROWS), f32),
            far_sds((16, 1, 2176), f32),
            far_sds((1024, E), bf16),
            far_sds((1024, 128), f32),
        ),
        where, *pairs, cols,
        in_specs=[smem] + [vm] * 5,
        out_specs=[vm, vm, vm, vm],
        scratch=[pltpu.VMEM((1024, 128), f32)],
        flops=10**9,
    )
    col_sums = exchange(col_sums, XZ)
    row_sums = kernel(pair_sum_body, sds((8, ROWS), f32), row_sums, swap(row_sums))
    row_sums = [row_sums] + [along_y(row_sums, -d) for d in (1, 2, 3)]
    scale = kernel(scale_body, sds((8 * ROWS, 128), f32), *row_sums)
    grads, mate_grads, loss = kernel(
        weight_body,
        (
            sds((4, ROWS, E), f32),
            sds((4, ROWS, E), f32),
            far_sds((1, 128), f32),
        ),
        where, kept(tile), kept(who), kept(cols), scale, col_sums,
        in_specs=[smem] + [vm] * 5,
        out_specs=[vm, vm, vm],
        scratch=[
            pltpu.VMEM((1024, E), f32),
        ],
        flops=3 * 10**9,
    )
    grads = kernel(add_body, (key_part,) * 4, grads, swap(mate_grads))
    mine = [grads[0]] + [along_y(grads[d], d) for d in (1, 2, 3)]
    raw_grad = kernel(raw_grad_body, sds((ROWS + 16, E), bf16), kept(raw), *mine, loss)
    ring = [raw_grad] + [along_y(raw_grad, -d) for d in (1, 2, 3)]
    zring = [along_z(raw_grad)] + [along_z(r) for r in ring[1:]]
    ring = ring + [swap(r) for r in ring]
    ring = ring + zring + [swap(r) for r in zring]
    ring_spec = pl.BlockSpec((ROWS + 16, E), lambda j: (0, 0))
    send, loss_all = kernel(
        head_body,
        (sds((8, U + 32, E), bf16), sds((1, 128), f32)),
        kept(joined_a), kept(joined_b), kept(hidden_a), kept(hidden_b), kept(slope_a), kept(slope_b), kept(w_second), *ring,
        grid=(2,),
        in_specs=[
            pl.BlockSpec((8 * ROWS, 1024), lambda j: (0, j)),
            pl.BlockSpec((8 * ROWS, 1024), lambda j: (0, j)),
            pl.BlockSpec((U, 8 * ROWS), lambda j: (0, 0)),
            pl.BlockSpec((U, 8 * ROWS), lambda j: (0, 0)),
            pl.BlockSpec((U, 8 * ROWS), lambda j: (0, 0)),
            pl.BlockSpec((U, 8 * ROWS), lambda j: (0, 0)),
            pl.BlockSpec((U, E), lambda j: (0, 0)),
        ]
        + [ring_spec] * 16,
        out_specs=[
            pl.BlockSpec((4, U + 32, E), lambda j: (j, 0, 0)),
            pl.BlockSpec((1, 128), lambda j: (0, 0)),
        ],
        scratch=[
            pltpu.VMEM((16 * ROWS, E), bf16),
            pltpu.VMEM((U, 16 * ROWS), bf16),
            pltpu.VMEM((U, E), bf16),
        ],
        flops=2 * 10**9,
    )
    got = exchange(send, BLK)
    piece = kernel(piece_body, sds((8, U + 32, E), bf16), got)
    whole = exchange(piece, BLK)
    first, second = kernel(
        final_body,
        (sds((C, U), f32), sds((U, E), f32)),
        whole,
        grid=(2,),
        in_specs=[pl.BlockSpec((4, U + 32, E), lambda j: (j, 0, 0))],
        out_specs=[
            pl.BlockSpec((1024, U), lambda j: (j, 0)),
            pl.BlockSpec((128, E), lambda j: (j, 0)),
        ],
    )
    return (loss_all[0, 0], first, second)


def solution(mesh):
    finer = Mesh(mesh.devices.reshape(4, 2, 2, 4, 2), ALL)
    placed = (P(ALL, None, None), P(ALL), P(ALL), P(None, GRP), P(GRP, None))
    return jax.shard_map(
        step,
        mesh=finer,
        in_specs=placed,
        out_specs=(P(), P(None, GRP), P(GRP, None)),
        check_vma=False,
    )
```
